32 devices in a mesh: gx: 8 (over z, y), gy: 4 (over x, core).
Axes of the slice: x: 2, y: 2, z: 4, core: 2. Of those that a mesh axis runs over, the one named last changes fastest.
Arguments:
- tokens: bfloat16 [256, 8192], P('gy', 'gx'), may hold values from -6 to 6
- target: bfloat16 [256, 8192], P('gy', 'gx'), may hold values from -6 to 6
- w_gate: bfloat16 [8192, 14336], P('gx', 'gy'), may hold values from -0.0625 to 0.0625
- w_up: bfloat16 [8192, 14336], P('gx', 'gy'), may hold values from -0.0625 to 0.0625
- w_down: bfloat16 [14336, 8192], P('gy', 'gx'), may hold values from -0.046875 to 0.046875
- t_gate: bfloat16 [8192, 14336], P('gx', 'gy'), may hold values from -0.0625 to 0.0625
- t_up: bfloat16 [8192, 14336], P('gx', 'gy'), may hold values from -0.0625 to 0.0625
- t_down: bfloat16 [14336, 8192], P('gy', 'gx'), may hold values from -0.046875 to 0.046875
Outputs:
- hvp_gate: bfloat16 [8192, 14336], P('gx', 'gy')
- hvp_up: bfloat16 [8192, 14336], P('gx', 'gy')
- hvp_down: bfloat16 [14336, 8192], P('gy', 'gx')
The draws below stay inside these ranges and needn't reach their ends.
All inputs are finite; a program needn't handle non-finite values.
Results may differ from the reference program's by a relative error of at most 0.0074.
Values may be sent and summed in bfloat16 or wider, within the bound.
A program may use at most 192 MiB of HBM per device.

```python
import math
import jax
import jax.numpy as jnp

D = 8192
FF = 14336
TOKENS = 256


def spiked(drawn, rng, source, target, blocks, factor):
    def block_of(position):
        return (jnp.arange(drawn.shape[position]) // (drawn.shape[position] // blocks)).reshape((-1,) + (1,) * (drawn.ndim - 1 - position))

    near = jax.random.permutation(rng, blocks)[block_of(target)]
    other_side = (block_of(target) + blocks // 2) % blocks
    return jnp.where((block_of(source) == near) | (block_of(source) == other_side), factor * drawn, drawn)


def levels(rng, extent, split, smallest, high):
    factor_of = 1.0
    for axis_at, parts in split:
        draws = jax.random.uniform(jax.random.fold_in(jax.random.fold_in(rng, 6), axis_at), (parts,), jnp.float32, smallest / len(split), high / len(split))
        factor_of = factor_of * jnp.repeat(jnp.exp(draws), extent[axis_at] // parts).reshape((-1,) + (1,) * (len(extent) - 1 - axis_at))
    return factor_of


def centred(own_key, extent, deviation, most, split=(), held_as=jnp.bfloat16):
    loudness = levels(own_key, extent, split, -0.22, 0.18) if split else 1.0
    result = jax.random.normal(own_key, extent, jnp.float32) * deviation * loudness
    return jnp.minimum(jnp.maximum(result, -most), most).astype(held_as)


def heavy_noise(stream_key, shape, spread, limit, shards, heavy, kind=jnp.bfloat16):
    array = spread * jax.random.normal(stream_key, shape, jnp.float32)
    if shards:
        array = array * levels(stream_key, shape, shards, -0.22, 0.18)
    return jnp.clip(spiked(array, jax.random.fold_in(stream_key, 3), *heavy), -limit, limit).astype(kind)


def setup_inputs(seed: int = 0) -> dict:
    key_of = jax.random.split(jax.random.key(seed), 9)
    tokens = heavy_noise(key_of[0], (TOKENS, D), 1.0, 6.0, ((0, 4), (1, 8)), (1, 0, 8, 2.0))
    target = centred(key_of[1], (TOKENS, D), 1.0, 6.0, ((0, 4), (1, 8)))
    w_gate = centred(key_of[2], (D, FF), D ** -0.5, 0.0625, ((0, 8), (1, 4)))
    w_up = centred(key_of[3], (D, FF), D ** -0.5, 0.0625, ((0, 8), (1, 4)))
    w_down = centred(key_of[4], (FF, D), FF ** -0.5, 0.046875, ((0, 4), (1, 8)))
    t_gate = centred(key_of[5], (D, FF), D ** -0.5, 0.0625, ((0, 8), (1, 4)))
    t_up = centred(key_of[6], (D, FF), D ** -0.5, 0.0625, ((0, 8), (1, 4)))
    t_down = centred(key_of[7], (FF, D), FF ** -0.5, 0.046875, ((0, 4), (1, 8)))
    return {"tokens": tokens, "target": target, "w_gate": w_gate, "w_up": w_up, "w_down": w_down, "t_gate": t_gate, "t_up": t_up, "t_down": t_down}


def silu_parts(gate):
    sig = jax.nn.sigmoid(gate)
    first = sig * (1.0 + gate * (1.0 - sig))
    second = sig * (1.0 - sig) * (2.0 + gate * (1.0 - 2.0 * sig))
    return (gate * sig, first, second)

def matmul(left, right):
    return jnp.dot(left, right, preferred_element_type=jnp.float32)

def reference(tokens, target, w_gate, w_up, w_down, t_gate, t_up, t_down):
    scale = 1.0 / math.sqrt(TOKENS)
    gate = matmul(tokens, w_gate)
    upper = matmul(tokens, w_up)
    gate_dot = matmul(tokens, t_gate)
    upper_dot = matmul(tokens, t_up)
    silu_val, first, second = silu_parts(gate)
    hidden = (silu_val * upper).astype(jnp.bfloat16)
    hidden_dot = (first * gate_dot * upper + silu_val * upper_dot).astype(jnp.bfloat16)
    output = matmul(hidden, w_down)
    output_dot = matmul(hidden_dot, w_down) + matmul(hidden, t_down)
    grad = ((output - target.astype(jnp.float32)) * scale).astype(jnp.bfloat16)
    grad_dot = (output_dot * scale).astype(jnp.bfloat16)
    hvp_down = (matmul(hidden_dot.T, grad) + matmul(hidden.T, grad_dot)).astype(jnp.bfloat16)
    back = matmul(grad, w_down.T)
    back_dot = matmul(grad_dot, w_down.T) + matmul(grad, t_down.T)
    gate_in = (back_dot * upper * first + back * upper_dot * first + back * upper * second * gate_dot).astype(jnp.bfloat16)
    upper_in = (back_dot * silu_val + back * first * gate_dot).astype(jnp.bfloat16)
    hvp_gate = matmul(tokens.T, gate_in).astype(jnp.bfloat16)
    hvp_up = matmul(tokens.T, upper_in).astype(jnp.bfloat16)
    return (hvp_gate, hvp_up, hvp_down)
```

```python
import functools
import math

import jax
import jax.numpy as jnp
from jax import lax
from jax.experimental import pallas as pl
from jax.experimental.pallas import tpu as pltpu
from jax.sharding import PartitionSpec as P

TOKENS = 256


def silu_parts(gate):
    sig = jax.nn.sigmoid(gate)
    first = sig * (1.0 + gate * (1.0 - sig))
    second = sig * (1.0 - sig) * (2.0 + gate * (1.0 - 2.0 * sig))
    return (gate * sig, first, second)


def matmul(left, right):
    return jnp.dot(left, right, preferred_element_type=jnp.float32)


def lead_dot(left, right):
    return lax.dot_general(
        left, right, (((0,), (0,)), ((), ())), preferred_element_type=jnp.float32
    )


def tail_dot(left, right):
    return lax.dot_general(
        left, right, (((1,), (1,)), ((), ())), preferred_element_type=jnp.float32
    )


def gather_kernel(axis, count, arrays, *refs):
    blocks, fulls = refs[:arrays], refs[arrays : 2 * arrays]
    own_sem, send, recv = refs[2 * arrays :]
    pairs = count // 2
    me = lax.axis_index(axis)
    side = lax.rem(me, 2)
    pair = lax.div(me, 2)
    partner = me + 1 - 2 * side
    peers = [lax.rem(pair + step, pairs) * 2 + side for step in range(1, pairs)]
    sources = [lax.rem(pair + pairs - step, pairs) * 2 + side for step in range(1, pairs)]
    rows = blocks[0].shape[0]

    def place(full, index):
        return full.at[pl.ds(pl.multiple_of(index * rows, rows), rows)]

    barrier = pltpu.get_barrier_semaphore()
    for peer in [partner, *peers]:
        pl.semaphore_signal(
            barrier, inc=1, device_id={axis: peer}, device_id_type=pl.DeviceIdType.MESH
        )
    pl.semaphore_wait(barrier, pairs)

    def remote(src, full, index, peer, slot):
        return pltpu.make_async_remote_copy(
            src_ref=src,
            dst_ref=place(full, index),
            send_sem=send.at[slot],
            recv_sem=recv.at[slot],
            device_id={axis: peer},
            device_id_type=pl.DeviceIdType.MESH,
        )

    slots = 2 * pairs - 1
    direct, final, own = {}, [], []
    for i in range(arrays):
        for step, peer in enumerate(peers):
            direct[i, step] = remote(blocks[i], fulls[i], me, peer, i * slots + step)
            direct[i, step].start()
        copy = remote(blocks[i], fulls[i], me, partner, i * slots + pairs - 1)
        copy.start()
        final.append(copy)
        own.append(pltpu.make_async_copy(blocks[i], place(fulls[i], me), own_sem.at[i]))
        own[-1].start()
    for i in range(arrays):
        for step, source in enumerate(sources):
            direct[i, step].wait_recv()
            copy = remote(
                place(fulls[i], source), fulls[i], source, partner, i * slots + pairs + step
            )
            copy.start()
            final.append(copy)
    for copy in direct.values():
        copy.wait_send()
    for copy in final + own:
        copy.wait()


def gather(blocks, axis, collective_id):
    count = lax.axis_size(axis)
    arrays = len(blocks)
    slots = arrays * (count - 1)
    sent = sum(block.size * 2 * (count - 1) for block in blocks)
    return pl.pallas_call(
        functools.partial(gather_kernel, axis, count, arrays),
        out_shape=[
            jax.ShapeDtypeStruct((count * block.shape[0], block.shape[1]), block.dtype)
            for block in blocks
        ],
        in_specs=[pl.BlockSpec(memory_space=pltpu.VMEM)] * arrays,
        out_specs=[pl.BlockSpec(memory_space=pl.ANY)] * arrays,
        scratch_shapes=[
            pltpu.SemaphoreType.DMA((arrays,)),
            pltpu.SemaphoreType.DMA((slots,)),
            pltpu.SemaphoreType.DMA((slots,)),
        ],
        compiler_params=pltpu.CompilerParams(
            collective_id=collective_id, has_side_effects=True
        ),
        cost_estimate=pl.CostEstimate(
            flops=0, bytes_accessed=16 * sent, transcendentals=0
        ),
    )(*blocks)


def products_kernel(turned, gate, upper, out_gate, out_up):
    out_gate[...] = matmul(turned[...], gate[...]).astype(out_gate.dtype)
    out_up[...] = matmul(turned[...], upper[...]).astype(out_up.dtype)


def weight_products(turned, gate, upper):
    rows, depth = turned.shape
    width = gate.shape[1]
    tile = next(size for size in (512, 256, 128) if width % size == 0)
    return pl.pallas_call(
        products_kernel,
        grid=(width // tile,),
        in_specs=[
            pl.BlockSpec((rows, depth), lambda i: (0, 0)),
            pl.BlockSpec((depth, tile), lambda i: (0, i)),
            pl.BlockSpec((depth, tile), lambda i: (0, i)),
        ],
        out_specs=[pl.BlockSpec((rows, tile), lambda i: (0, i))] * 2,
        out_shape=[jax.ShapeDtypeStruct((rows, width), jnp.bfloat16)] * 2,
        cost_estimate=pl.CostEstimate(
            flops=4 * rows * depth * width,
            bytes_accessed=4 * (rows + depth) * width,
            transcendentals=0,
        ),
    )(turned, gate, upper)


def scatter_kernel(axis, count, arrays, *refs):
    parts, outs = refs[:arrays], refs[arrays : 2 * arrays]
    landed, held, got, send1, recv1, send2, recv2 = refs[2 * arrays :]
    pairs = count // 2
    me = lax.axis_index(axis)
    side = lax.rem(me, 2)
    pair = lax.div(me, 2)
    partner = me + 1 - 2 * side
    targets = [lax.rem(pair + step, pairs) * 2 for step in range(1, pairs)]
    peers = [target + side for target in targets]

    barrier = pltpu.get_barrier_semaphore()
    for peer in [partner, *peers]:
        pl.semaphore_signal(
            barrier, inc=1, device_id={axis: peer}, device_id_type=pl.DeviceIdType.MESH
        )
    pl.semaphore_wait(barrier, pairs)

    first = {}
    for i in range(arrays):
        for k, target in enumerate([*targets, pair * 2]):
            first[i, k] = pltpu.make_async_remote_copy(
                src_ref=parts[i].at[target + 1 - side],
                dst_ref=landed.at[i, k],
                send_sem=send1.at[i * pairs + k],
                recv_sem=recv1.at[i * pairs + k],
                device_id={axis: partner},
                device_id_type=pl.DeviceIdType.MESH,
            )
            first[i, k].start()
    second = {}
    for i in range(arrays):
        for k, target in enumerate([*targets, pair * 2]):
            first[i, k].wait_recv()
            term = parts[i][target + side].astype(jnp.float32) + landed[i, k].astype(jnp.float32)
            if k == pairs - 1:
                outs[i][...] = term
                continue
            held[i, k] = term.astype(held.dtype)
            second[i, k] = pltpu.make_async_remote_copy(
                src_ref=held.at[i, k],
                dst_ref=got.at[i, k],
                send_sem=send2.at[i * pairs + k],
                recv_sem=recv2.at[i * pairs + k],
                device_id={axis: peers[k]},
                device_id_type=pl.DeviceIdType.MESH,
            )
            second[i, k].start()
    for i in range(arrays):
        for k in range(pairs - 1):
            second[i, k].wait_recv()
            outs[i][...] += got[i, k].astype(jnp.float32)
    for copy in [*first.values(), *second.values()]:
        copy.wait_send()


def scatter_sum(partials, axis, collective_id):
    count = lax.axis_size(axis)
    pairs = count // 2
    arrays = len(partials)
    rows, columns = partials[0].shape[0] // count, partials[0].shape[1]
    parts = [p.astype(jnp.bfloat16).reshape(count, rows, columns) for p in partials]
    sent = 2 * rows * columns * arrays * (count - 1)
    return pl.pallas_call(
        functools.partial(scatter_kernel, axis, count, arrays),
        out_shape=[jax.ShapeDtypeStruct((rows, columns), jnp.float32)] * arrays,
        in_specs=[pl.BlockSpec(memory_space=pltpu.VMEM)] * arrays,
        out_specs=[pl.BlockSpec(memory_space=pltpu.VMEM)] * arrays,
        scratch_shapes=[
            pltpu.VMEM((arrays, pairs, rows, columns), jnp.bfloat16),
            pltpu.VMEM((arrays, max(pairs - 1, 1), rows, columns), jnp.bfloat16),
            pltpu.VMEM((arrays, max(pairs - 1, 1), rows, columns), jnp.bfloat16),
            *[pltpu.SemaphoreType.DMA((arrays * pairs,))] * 4,
        ],
        compiler_params=pltpu.CompilerParams(
            collective_id=collective_id, has_side_effects=True
        ),
        cost_estimate=pl.CostEstimate(flops=0, bytes_accessed=16 * sent, transcendentals=0),
    )(*parts)


def ring_width(width):
    return next(size for size in (256, 128) if width % size == 0)


def between(value, low, high):
    return jnp.logical_and(value >= low, value < high)


def stream_kernel(axis, plan, *refs):
    count, rows, width, chunk = plan.count, plan.rows, plan.width, plan.chunk
    line, group, steps = count // 2, rows // 4, width // chunk
    last = line - 1
    ins, outs = refs[: plan.n_ins], refs[plan.n_ins : plan.n_ins + plan.n_outs]
    rest = refs[plan.n_ins + plan.n_outs :]
    (part, y_out, y_in, a_out, a_in, b_out, b_in, f_out, f_in) = rest[:9]
    (y_s, y_r, a_s, a_r, b_s, b_r, f_s, f_r, h_s, h_r, g_s, g_r, x_s, x_r, k_s, k_r) = rest[9:25]
    extra = rest[25:]
    full0, full1 = outs[0], outs[1]
    na, nb = plan.pair_first, plan.line_first

    me = lax.axis_index(axis)
    spot = lax.div(me, 2)
    side = lax.rem(me, 2)
    partner = me + 1 - 2 * side
    at_end = jnp.logical_or(spot == 0, spot == last)
    end = jnp.where(spot == 0, 0, 1)
    place = [last - spot, spot]

    barrier = pltpu.get_barrier_semaphore()

    def greet(peer):
        pl.semaphore_signal(
            barrier, inc=1, device_id={axis: peer}, device_id_type=pl.DeviceIdType.MESH
        )

    greet(partner)
    pl.when(spot > 0)(lambda: greet(me - 2))
    pl.when(spot < last)(lambda: greet(me + 2))
    work = plan.setup(ins, outs, extra)
    pl.semaphore_wait(barrier, jnp.where(at_end, 2, 3))

    def remote(src, dst, send, recv, peer):
        return pltpu.make_async_remote_copy(
            src_ref=src,
            dst_ref=dst,
            send_sem=send,
            recv_sem=recv,
            device_id={axis: peer},
            device_id_type=pl.DeviceIdType.MESH,
        )

    def rows_of(e, s):
        return pl.ds(pl.multiple_of((e * 2 + s) * group, group), group)

    def cols_of(j):
        return pl.ds(pl.multiple_of(j * chunk, chunk), chunk)

    def y_copy(j):
        return remote(y_out.at[j], y_in.at[j], y_s.at[j], y_r.at[j], partner)

    def a_copy(d, j):
        return remote(a_out.at[d, j], a_in.at[d, j], a_s.at[d, j], a_r.at[d, j], me - 2 + 4 * d)

    def b_copy(d, j):
        return remote(b_out.at[d, j], b_in.at[d, j], b_s.at[d, j], b_r.at[d, j], me - 2 + 4 * d)

    def f_copy(j):
        return remote(f_out.at[j], f_in.at[j], f_s.at[j], f_r.at[j], partner)

    def h_copy(d, j):
        block = full0.at[rows_of(1 - d, side), cols_of(j)]
        return remote(block, block, h_s.at[d, j], h_r.at[d, j], me - 2 + 4 * d)

    def g_copy(d, j):
        block = full0.at[rows_of(1 - d, side), cols_of(j)]
        return remote(block, block, g_s.at[d, j], g_r.at[d, j], partner)

    def x_copy(j):
        block = full1.at[rows_of(end, side), cols_of(j)]
        return remote(block, block, x_s.at[j], x_r.at[j], partner)

    def k_copy(d, j):
        block = full1.at[pl.ds((1 - d) * 2 * group, 2 * group), cols_of(j)]
        return remote(block, block, k_s.at[d, j], k_r.at[d, j], me - 2 + 4 * d)

    def step(t, carry):
        for d in (0, 1):
            p = place[d]
            jk = t - line - 1 - p
            go = between(jk, 0, steps)

            @pl.when(jnp.logical_and(go, p > 0))
            def _():
                k_copy(d, jk).wait_recv()

            @pl.when(jnp.logical_and(go, p == 0))
            def _():
                x_copy(jk).wait_recv()

            @pl.when(jnp.logical_and(go, p < last))
            def _():
                k_copy(d, jk).start()

            jh = t - line - p

            @pl.when(jnp.logical_and(between(jh, 0, steps), p > 0))
            def _():
                h_copy(d, jh).wait_recv()
                g_copy(d, jh).start()

            @pl.when(jnp.logical_and(between(jh, 0, steps), between(p, 1, last)))
            def _():
                h_copy(d, jh).start()

            @pl.when(go)
            def _():
                g_copy(d, jk).wait_recv()

        jc = t - line

        @pl.when(jnp.logical_and(between(jc, 0, steps), at_end))
        def _():
            a_copy(end, jc).wait_recv()
            f_copy(jc).wait_recv()
            mine = rows_of(end, side)
            sums = [None] * (len(na) + len(nb))
            for i, a in enumerate(na):
                sums[a] = part[a, jc, mine, :] + a_in[end, jc, i].astype(jnp.float32)
            for i, a in enumerate(nb):
                sums[a] = part[a, jc, mine, :] + f_in[jc, i].astype(jnp.float32)
            first, second = plan.combine(ins, outs, cols_of(jc), sums)
            full0[mine, cols_of(jc)] = first
            full1[mine, cols_of(jc)] = second
            x_copy(jc).start()

        for d in (0, 1):

            @pl.when(jnp.logical_and(between(jc, 0, steps), place[d] == 0))
            def _():
                h_copy(d, jc).start()
                g_copy(d, jc).start()

        for d in (0, 1):
            p = place[d]
            jb = t - p
            slab = pl.ds(d * 2 * group, 2 * group)

            @pl.when(jnp.logical_and(between(jb, 0, steps), between(p, 1, last)))
            def _():
                b_copy(d, jb).wait_recv()
                for i, a in enumerate(nb):
                    b_out[d, jb, i] = (
                        part[a, jb, slab, :] + b_in[d, jb, i].astype(jnp.float32)
                    ).astype(jnp.bfloat16)
                b_copy(d, jb).start()

            @pl.when(jnp.logical_and(between(jb, 0, steps), p == last))
            def _():
                b_copy(d, jb).wait_recv()
                own = pl.ds(pl.multiple_of(side * group, group), group)
                other = pl.ds(pl.multiple_of((1 - side) * group, group), group)
                for i, a in enumerate(nb):
                    f_out[jb, i] = (
                        part[a, jb, rows_of(d, 1 - side), :]
                        + b_in[d, jb, i, other, :].astype(jnp.float32)
                    ).astype(jnp.bfloat16)
                f_copy(jb).start()
                for i, a in enumerate(nb):
                    part[a, jb, rows_of(d, side), :] += b_in[d, jb, i, own, :].astype(jnp.float32)

        jy = t - 1

        @pl.when(between(jy, 0, steps))
        def _():
            y_copy(jy).wait_recv()
            for i, a in enumerate(na):
                for e in (0, 1):
                    part[a, jy, rows_of(e, side), :] += y_in[jy, i, e].astype(jnp.float32)

        for d in (0, 1):
            p = place[d]
            ja = t - 1 - p

            @pl.when(jnp.logical_and(between(ja, 0, steps), between(p, 1, last)))
            def _():
                a_copy(d, ja).wait_recv()
                for i, a in enumerate(na):
                    a_out[d, ja, i] = (
                        part[a, ja, rows_of(d, side), :] + a_in[d, ja, i].astype(jnp.float32)
                    ).astype(jnp.bfloat16)
                a_copy(d, ja).start()

            @pl.when(jnp.logical_and(between(ja, 0, steps), p == 0))
            def _():
                for i, a in enumerate(na):
                    a_out[d, ja, i] = part[a, ja, rows_of(d, side), :].astype(jnp.bfloat16)
                a_copy(d, ja).start()

        @pl.when(t < steps)
        def _():
            plan.produce(work, t, part)
            for i, a in enumerate(na):
                for e in (0, 1):
                    y_out[t, i, e] = part[a, t, rows_of(e, 1 - side), :].astype(jnp.bfloat16)
            y_copy(t).start()

        for d in (0, 1):

            @pl.when(jnp.logical_and(t < steps, place[d] == 0))
            def _():
                for i, a in enumerate(nb):
                    b_out[d, t, i] = part[a, t, pl.ds(d * 2 * group, 2 * group), :].astype(
                        jnp.bfloat16
                    )
                b_copy(d, t).start()

        if plan.consume is not None:
            jd = t - 2 * line

            @pl.when(between(jd, 0, steps))
            def _():
                plan.consume(work, jd, full0, full1)

        return carry

    lax.fori_loop(0, steps + 2 * line, step, 0)

    def settle(j, carry):
        y_copy(j).wait_send()

        @pl.when(at_end)
        def _():
            f_copy(j).wait_send()
            x_copy(j).wait_send()

        for d in (0, 1):
            g_copy(d, j).wait_send()

            @pl.when(place[d] < last)
            def _():
                a_copy(d, j).wait_send()
                b_copy(d, j).wait_send()
                h_copy(d, j).wait_send()
                k_copy(d, j).wait_send()

        return carry

    lax.fori_loop(0, steps, settle, 0)
    if plan.finish is not None:
        plan.finish(work, outs)


class Plan:
    def __init__(self, **fields):
        self.__dict__.update(fields)


def stream(plan, axis, collective_id, operands, in_specs, more_outs, more_scratch, flops):
    count, rows, width, chunk = plan.count, plan.rows, plan.width, plan.chunk
    group, steps = rows // 4, width // chunk
    na, nb = len(plan.pair_first), len(plan.line_first)
    vmem = pl.BlockSpec(memory_space=pltpu.VMEM)
    full = jax.ShapeDtypeStruct((rows, width), jnp.bfloat16)
    outs = [full, full, *more_outs]
    plan.n_ins, plan.n_outs = len(operands), len(outs)

    def travel(*shape):
        return [pltpu.VMEM(shape, jnp.bfloat16)] * 2

    def marks(*shape):
        return [pltpu.SemaphoreType.DMA(shape)] * 2

    return pl.pallas_call(
        functools.partial(stream_kernel, axis, plan),
        out_shape=outs,
        in_specs=in_specs,
        out_specs=[vmem] * len(outs),
        scratch_shapes=[
            pltpu.VMEM((na + nb, steps, rows, chunk), jnp.float32),
            *travel(steps, na, 2, group, chunk),
            *travel(2, steps, na, group, chunk),
            *travel(2, steps, nb, 2 * group, chunk),
            *travel(steps, nb, group, chunk),
            *marks(steps),
            *marks(2, steps),
            *marks(2, steps),
            *marks(steps),
            *marks(2, steps),
            *marks(2, steps),
            *marks(steps),
            *marks(2, steps),
            *more_scratch,
        ],
        compiler_params=pltpu.CompilerParams(
            collective_id=collective_id, has_side_effects=True, vmem_limit_bytes=67043328
        ),
        cost_estimate=pl.CostEstimate(
            flops=flops, bytes_accessed=40 * rows * width, transcendentals=0
        ),
    )(*operands)


class Feed:
    def __init__(self, sources, slots, sems, steps, view):
        self.sources, self.slots, self.sems = sources, slots, sems
        self.steps, self.view = steps, view
        for j in range(min(2, steps)):
            for copy in self.copies(j):
                copy.start()

    def copies(self, j):
        slot = lax.rem(j, 3)
        return [
            pltpu.make_async_copy(
                self.view(source, j), self.slots.at[slot, i], self.sems.at[slot, i]
            )
            for i, source in enumerate(self.sources)
        ]

    def take(self, j):
        for copy in self.copies(j):
            copy.wait()

        @pl.when(j + 2 < self.steps)
        def _():
            for copy in self.copies(j + 2):
                copy.start()

        return self.slots.at[lax.rem(j, 3)]


def forward(x, w_gate, w_up, t_gate, t_up, w_down, t_down):
    count = lax.axis_size("gx")
    rows, depth = x.shape
    width = w_gate.shape[1]
    model = w_down.shape[1]
    chunk = ring_width(width)
    steps, group = width // chunk, rows // 4

    def setup(ins, outs, extra):
        up_slots, up_sems, down_slots, down_sems, totals = extra
        up = Feed(
            ins[1:5],
            up_slots,
            up_sems,
            steps,
            lambda ref, j: ref.at[:, pl.ds(pl.multiple_of(j * chunk, chunk), chunk)],
        )
        down = Feed(
            ins[5:7],
            down_slots,
            down_sems,
            steps,
            lambda ref, j: ref.at[pl.ds(pl.multiple_of(j * chunk, chunk), chunk), :],
        )
        totals[...] = jnp.zeros_like(totals)
        return ins[0], up, down, totals

    def produce(work, j, part):
        x_ref, up, _, _ = work
        weights = up.take(j)
        for i in range(4):
            part[i, j] = matmul(x_ref[...], weights[i])

    def combine(ins, outs, columns, sums):
        for i in range(4):
            outs[2][i, :, columns] = sums[i]
        gate, upper, gate_dot, upper_dot = sums
        silu_val, first, _ = silu_parts(gate)
        hidden = (silu_val * upper).astype(jnp.bfloat16)
        hidden_dot = (first * gate_dot * upper + silu_val * upper_dot).astype(jnp.bfloat16)
        return hidden, hidden_dot

    def consume(work, j, full0, full1):
        _, _, down, totals = work
        weights = down.take(j)
        columns = pl.ds(pl.multiple_of(j * chunk, chunk), chunk)
        hidden, hidden_dot = full0[:, columns], full1[:, columns]
        totals[0] += matmul(hidden, weights[0])
        totals[1] += matmul(hidden_dot, weights[0]) + matmul(hidden, weights[1])

    def finish(work, outs):
        totals = work[3]
        outs[3][...] = totals[0].astype(jnp.bfloat16)
        outs[4][...] = totals[1].astype(jnp.bfloat16)

    plan = Plan(
        count=count, rows=rows, width=width, chunk=chunk,
        pair_first=(0, 2), line_first=(1, 3),
        setup=setup, produce=produce, combine=combine, consume=consume, finish=finish,
    )
    any_spec = pl.BlockSpec(memory_space=pl.ANY)
    return stream(
        plan, "gx", 1,
        [x, w_gate, w_up, t_gate, t_up, w_down, t_down],
        [pl.BlockSpec(memory_space=pltpu.VMEM)] + [any_spec] * 6,
        [
            jax.ShapeDtypeStruct((4, group, width), jnp.float32),
            jax.ShapeDtypeStruct((rows, model), jnp.bfloat16),
            jax.ShapeDtypeStruct((rows, model), jnp.bfloat16),
        ],
        [
            pltpu.VMEM((3, 4, depth, chunk), jnp.bfloat16),
            pltpu.SemaphoreType.DMA((3, 4)),
            pltpu.VMEM((3, 2, chunk, model), jnp.bfloat16),
            pltpu.SemaphoreType.DMA((3, 2)),
            pltpu.VMEM((2, rows, model), jnp.float32),
        ],
        14 * rows * depth * width,
    )


def backward(grad, grad_dot, w_down, t_down, sums):
    count = lax.axis_size("gx")
    rows, model = grad.shape
    width = w_down.shape[0]
    chunk = ring_width(width)
    steps = width // chunk

    def setup(ins, outs, extra):
        slots, sems = extra
        feed = Feed(
            ins[2:4],
            slots,
            sems,
            steps,
            lambda ref, j: ref.at[pl.ds(pl.multiple_of(j * chunk, chunk), chunk), :],
        )
        return ins[0], ins[1], feed

    def produce(work, j, part):
        grad_ref, grad_dot_ref, feed = work
        weights = feed.take(j)
        part[0, j] = tail_dot(grad_ref[...], weights[0])
        part[1, j] = tail_dot(grad_dot_ref[...], weights[0]) + tail_dot(grad_ref[...], weights[1])

    def combine(ins, outs, columns, arrived):
        back, back_dot = arrived
        gate, upper, gate_dot, upper_dot = [ins[4][i, :, columns] for i in range(4)]
        silu_val, first, second = silu_parts(gate)
        gate_in = (
            back_dot * upper * first + back * upper_dot * first + back * upper * second * gate_dot
        ).astype(jnp.bfloat16)
        upper_in = (back_dot * silu_val + back * first * gate_dot).astype(jnp.bfloat16)
        return gate_in, upper_in

    plan = Plan(
        count=count, rows=rows, width=width, chunk=chunk,
        pair_first=(0,), line_first=(1,),
        setup=setup, produce=produce, combine=combine, consume=None, finish=None,
    )
    vmem, any_spec = pl.BlockSpec(memory_space=pltpu.VMEM), pl.BlockSpec(memory_space=pl.ANY)
    return stream(
        plan, "gx", 3,
        [grad, grad_dot, w_down, t_down, sums],
        [vmem, vmem, any_spec, any_spec, vmem],
        [],
        [
            pltpu.VMEM((3, 2, chunk, model), jnp.bfloat16),
            pltpu.SemaphoreType.DMA((3, 2)),
        ],
        6 * rows * model * width,
    )


def body(tokens, target, w_gate, w_up, w_down, t_gate, t_up, t_down):
    scale = 1.0 / math.sqrt(TOKENS)
    (xfull,) = gather([tokens], "gy", 0)
    hid_full, hid_dot_full, sums, output, output_dot = forward(
        xfull, w_gate, w_up, t_gate, t_up, w_down, t_down
    )
    output, output_dot = scatter_sum([output, output_dot], "gy", 6)
    grad = ((output - target.astype(jnp.float32)) * scale).astype(jnp.bfloat16)
    grad_dot = (output_dot * scale).astype(jnp.bfloat16)
    grad_full, grad_dot_full = gather([grad, grad_dot], "gy", 2)
    hvp_down = (lead_dot(hid_dot_full, grad_full) + lead_dot(hid_full, grad_dot_full)).astype(
        jnp.bfloat16
    )
    gate_full, upper_full = backward(grad_full, grad_dot_full, w_down, t_down, sums)
    hvp_gate, hvp_up = weight_products(lax.optimization_barrier(xfull.T), gate_full, upper_full)
    return (hvp_gate, hvp_up, hvp_down)


def solution(mesh):
    return jax.shard_map(
        body,
        mesh=mesh,
        in_specs=(
            P("gy", "gx"),
            P("gy", "gx"),
            P("gx", "gy"),
            P("gx", "gy"),
            P("gy", "gx"),
            P("gx", "gy"),
            P("gx", "gy"),
            P("gy", "gx"),
        ),
        out_specs=(P("gx", "gy"), P("gx", "gy"), P("gy", "gx")),
        check_vma=False,
    )
```

```python
import functools
import math

import jax
import jax.numpy as jnp
from jax import lax
from jax.experimental import pallas as pl
from jax.experimental.pallas import tpu as pltpu
from jax.sharding import PartitionSpec as P

TOKENS = 256
CHUNKS = (512, 256, 128)
F32, BF16 = jnp.float32, jnp.bfloat16


def silu_parts(gate):
    sig = jax.nn.sigmoid(gate)
    first = sig * (1.0 + gate * (1.0 - sig))
    second = sig * (1.0 - sig) * (2.0 + gate * (1.0 - 2.0 * sig))
    return (gate * sig, first, second)


def matmul(left, right):
    return jnp.dot(left, right, preferred_element_type=F32)


def lead_dot(left, right):
    return lax.dot_general(left, right, (((0,), (0,)), ((), ())), preferred_element_type=F32)


def tail_dot(left, right):
    return lax.dot_general(left, right, (((1,), (1,)), ((), ())), preferred_element_type=F32)


def between(value, low, high):
    return jnp.logical_and(value >= low, value < high)


def both(*terms):
    return functools.reduce(jnp.logical_and, terms)


def span(start, size):
    return pl.ds(pl.multiple_of(start * size, size), size)


def remote(src, dst, sems, index, axis, peer):
    return pltpu.make_async_remote_copy(
        src_ref=src,
        dst_ref=dst,
        send_sem=sems[0].at[index],
        recv_sem=sems[1].at[index],
        device_id={axis: peer},
        device_id_type=pl.DeviceIdType.MESH,
    )


class Sizes:
    def __init__(self, tokens, w_gate):
        self.line = lax.axis_size("gx") // 2
        self.gy = lax.axis_size("gy")
        self.pairs = self.gy // 2
        own, self.depth = tokens.shape
        self.width = w_gate.shape[1]
        self.halves = 2 if own % 32 == 0 else 1
        self.own = own // self.halves
        self.rows = self.own * self.gy
        self.group = self.rows // 4
        self.chunk = next(size for size in CHUNKS if self.width % size == 0)
        self.steps = self.width // self.chunk
        self.items = self.halves * self.steps


class Stream:
    def __init__(self, sizes, na, nb):
        self.z, self.na, self.nb = sizes, na, nb

    def scratch(self):
        z, na, nb = self.z, self.na, self.nb
        n, g, c = z.items, z.group, z.chunk
        sem = pltpu.SemaphoreType.DMA
        pairs = [(n,), (2, n), (2, n), (n,), (2, n), (2, n), (n,), (2, n)]
        return [
            pltpu.VMEM((na + nb, z.line, z.rows, c), F32),
            pltpu.VMEM((n, na, 2, g, c), BF16),
            pltpu.VMEM((n, na, 2, g, c), BF16),
            pltpu.VMEM((2, n, na, g, c), BF16),
            pltpu.VMEM((2, n, nb, 2 * g, c), BF16),
            pltpu.VMEM((n, nb, g, c), BF16),
            pltpu.VMEM((n, nb, g, c), BF16),
            *[sem(shape) for shape in pairs for _ in range(2)],
        ]

    def bind(self, refs, full0, full1, produce, combine, consume):
        self.part, self.y_out, self.y_in, self.a, self.b, self.f_out, self.f_in = refs[:7]
        sems = [(refs[7 + 2 * i], refs[8 + 2 * i]) for i in range(8)]
        (self.ys, self.as_, self.bs, self.fs, self.hs, self.gs, self.xs, self.ks) = sems
        self.full0, self.full1 = full0, full1
        self.produce, self.combine, self.consume = produce, combine, consume
        z = self.z
        self.me = lax.axis_index("gx")
        self.spot, self.side = lax.div(self.me, 2), lax.rem(self.me, 2)
        self.partner = self.me + 1 - 2 * self.side
        self.last = z.line - 1
        self.at_end = jnp.logical_or(self.spot == 0, self.spot == self.last)
        self.end = jnp.where(self.spot == 0, 0, 1)
        self.place = [self.last - self.spot, self.spot]

    def group_of(self, e, s):
        return span(e * 2 + s, self.z.group)

    def block(self, full, k, e, s):
        z = self.z
        half, j = lax.div(k, z.steps), lax.rem(k, z.steps)
        return full.at[span(half * 4 + e * 2 + s, z.group), span(j, z.chunk)]

    def slab(self, full, k, e):
        z = self.z
        half, j = lax.div(k, z.steps), lax.rem(k, z.steps)
        return full.at[span(half * 2 + e, 2 * z.group), span(j, z.chunk)]

    def across(self, src, dst, sems, index):
        return remote(src, dst, sems, index, "gx", self.partner)

    def along(self, d, src, dst, sems, index):
        return remote(src, dst, sems, index, "gx", self.me - 2 + 4 * d)

    def y_copy(self, k):
        return self.across(self.y_out.at[k], self.y_in.at[k], self.ys, k)

    def f_copy(self, k):
        return self.across(self.f_out.at[k], self.f_in.at[k], self.fs, k)

    def a_copy(self, d, k):
        return self.along(d, self.a.at[d, k], self.a.at[d, k], self.as_, (d, k))

    def b_copy(self, d, k):
        return self.along(d, self.b.at[d, k], self.b.at[d, k], self.bs, (d, k))

    def h_copy(self, d, k):
        block = self.block(self.full0, k, 1 - d, self.side)
        return self.along(d, block, block, self.hs, (d, k))

    def g_copy(self, d, k):
        block = self.block(self.full0, k, 1 - d, self.side)
        return self.across(block, block, self.gs, (d, k))

    def x_copy(self, k):
        block = self.block(self.full1, k, self.end, self.side)
        return self.across(block, block, self.xs, k)

    def k_copy(self, d, k):
        block = self.slab(self.full1, k, 1 - d)
        return self.along(d, block, block, self.ks, (d, k))

    def early(self, t):
        z, last, side, na, nb = self.z, self.last, self.side, self.na, self.nb
        n, part, a, b = z.items, self.part, self.a, self.b
        for d in (0, 1):
            p = self.place[d]
            k, h = t - z.line - 1 - p, t - z.line - p
            go = between(k, 0, n)

            @pl.when(both(go, p > 0))
            def _():
                self.k_copy(d, k).wait_recv()

            @pl.when(both(go, p == 0))
            def _():
                self.x_copy(k).wait_recv()

            @pl.when(both(go, p < last))
            def _():
                self.k_copy(d, k).start()

            @pl.when(both(between(h, 0, n), p > 0))
            def _():
                self.h_copy(d, h).wait_recv()
                self.g_copy(d, h).start()

            @pl.when(both(between(h, 0, n), between(p, 1, last)))
            def _():
                self.h_copy(d, h).start()

            @pl.when(go)
            def _():
                self.g_copy(d, k).wait_recv()

        k = t - z.line

        @pl.when(both(between(k, 0, n), self.at_end))
        def _():
            self.a_copy(self.end, k).wait_recv()
            self.f_copy(k).wait_recv()
            slot, mine = lax.rem(k, z.line), self.group_of(self.end, side)
            sums = [part[i, slot, mine, :] + a[self.end, k, i].astype(F32) for i in range(na)]
            sums += [part[na + i, slot, mine, :] + self.f_in[k, i].astype(F32) for i in range(nb)]
            first, second = self.combine(k, sums)
            self.block(self.full0, k, self.end, side)[...] = first
            self.block(self.full1, k, self.end, side)[...] = second
            self.x_copy(k).start()
            self.h_copy(1 - self.end, k).start()
            self.g_copy(1 - self.end, k).start()

        for d in (0, 1):
            p = self.place[d]
            k = t - p

            @pl.when(both(between(k, 0, n), between(p, 1, last)))
            def _():
                self.b_copy(d, k).wait_recv()
                slot, slab = lax.rem(k, z.line), span(d, 2 * z.group)
                for i in range(nb):
                    b[d, k, i] = (part[na + i, slot, slab, :] + b[d, k, i].astype(F32)).astype(BF16)
                self.b_copy(d, k).start()

            @pl.when(both(between(k, 0, n), p == last))
            def _():
                self.b_copy(d, k).wait_recv()
                slot = lax.rem(k, z.line)
                own, other = span(side, z.group), span(1 - side, z.group)
                for i in range(nb):
                    self.f_out[k, i] = (
                        part[na + i, slot, self.group_of(d, 1 - side), :]
                        + b[d, k, i, other, :].astype(F32)
                    ).astype(BF16)
                self.f_copy(k).start()
                for i in range(nb):
                    part[na + i, slot, self.group_of(d, side), :] += b[d, k, i, own, :].astype(F32)

        k = t - 1

        @pl.when(between(k, 0, n))
        def _():
            self.y_copy(k).wait_recv()
            for i in range(na):
                for e in (0, 1):
                    part[i, lax.rem(k, z.line), self.group_of(e, side), :] += self.y_in[
                        k, i, e
                    ].astype(F32)

        for d in (0, 1):
            p = self.place[d]
            k = t - 1 - p

            @pl.when(both(between(k, 0, n), between(p, 1, last)))
            def _():
                self.a_copy(d, k).wait_recv()
                for i in range(na):
                    a[d, k, i] = (
                        part[i, lax.rem(k, z.line), self.group_of(d, side), :]
                        + a[d, k, i].astype(F32)
                    ).astype(BF16)
                self.a_copy(d, k).start()

            @pl.when(both(between(k, 0, n), p == 0))
            def _():
                for i in range(na):
                    a[d, k, i] = part[i, lax.rem(k, z.line), self.group_of(d, side), :].astype(BF16)
                self.a_copy(d, k).start()

    def late(self, t):
        z, na, nb = self.z, self.na, self.nb

        @pl.when(between(t, 0, z.items))
        def _():
            slot = lax.rem(t, z.line)
            self.produce(t, self.part, slot)
            for i in range(na):
                for e in (0, 1):
                    self.y_out[t, i, e] = self.part[
                        i, slot, self.group_of(e, 1 - self.side), :
                    ].astype(BF16)
            self.y_copy(t).start()

            @pl.when(self.at_end)
            def _():
                d = 1 - self.end
                for i in range(nb):
                    self.b[d, t, i] = self.part[na + i, slot, span(d, 2 * z.group), :].astype(BF16)
                self.b_copy(d, t).start()

        if self.consume is not None:
            k = t - 2 * z.line

            @pl.when(between(k, 0, z.items))
            def _():
                self.consume(k)

    def settle(self, k):
        self.y_copy(k).wait_send()

        @pl.when(self.at_end)
        def _():
            self.f_copy(k).wait_send()
            self.x_copy(k).wait_send()

        for d in (0, 1):
            self.g_copy(d, k).wait_send()

            @pl.when(self.place[d] < self.last)
            def _():
                self.a_copy(d, k).wait_send()
                self.b_copy(d, k).wait_send()
                self.h_copy(d, k).wait_send()
                self.k_copy(d, k).wait_send()


class Feed:
    def __init__(self, sources, slots, sems, sizes, view):
        self.sources, self.slots, self.sems = sources, slots, sems
        self.sizes, self.view = sizes, view

    def copies(self, k):
        slot, j = lax.rem(k, 2), lax.rem(k, self.sizes.steps)
        return [
            pltpu.make_async_copy(
                self.view(source, j), self.slots.at[slot, i], self.sems.at[slot, i]
            )
            for i, source in enumerate(self.sources)
        ]

    def start(self, k):
        for copy in self.copies(k):
            copy.start()

    def take(self, k):
        for copy in self.copies(k):
            copy.wait()
        pl.when(k + 1 < self.sizes.items)(lambda: self.start(k + 1))
        return self.slots.at[lax.rem(k, 2)]


def hvp_kernel(z, scale, forward, backward, *refs):
    tokens, target, w_gate, w_up, t_gate, t_up, w_down, t_down = refs[:8]
    x_full, hid, hid_dot, grads, gate_in, upper_in = refs[8:14]
    count = len(forward.scratch())
    f_refs, b_refs, rest = refs[14 : 14 + count], refs[14 + count : 14 + 2 * count], refs[14 + 2 * count :]
    up_slots, up_sems, down_slots, down_sems, back_slots, back_sems = rest[:6]
    totals, saved, m1_out, m1_in, m2_out, m2_in = rest[6:12]
    sems = [(rest[12 + 2 * i], rest[13 + 2 * i]) for i in range(8)]
    x1, x2, x3, m1, m2, m3, m3p, m4 = sems

    me = lax.axis_index("gy")
    core, pair = lax.rem(me, 2), lax.div(me, 2)
    other = me + 1 - 2 * core
    peers = [lax.rem(pair + s, z.pairs) * 2 + core for s in range(1, z.pairs)]
    sources = [lax.rem(pair + z.pairs - s, z.pairs) * 2 + core for s in range(1, z.pairs)]
    hops = range(z.pairs - 1)

    up = Feed((w_gate, w_up, t_gate, t_up), up_slots, up_sems, z, lambda r, j: r.at[:, span(j, z.chunk)])
    down = Feed((w_down, t_down), down_slots, down_sems, z, lambda r, j: r.at[span(j, z.chunk), :])
    again = Feed((w_down, t_down), back_slots, back_sems, z, lambda r, j: r.at[span(j, z.chunk), :])

    def half_rows(k):
        return span(lax.div(k, z.steps), z.rows)

    def produce_up(k, part, slot):
        weights = up.take(k)
        x = x_full[half_rows(k), :]
        for i in range(4):
            part[i, slot] = matmul(x, weights[(0, 2, 1, 3)[i]])

    def combine_up(k, sums):
        gate, gate_dot, upper, upper_dot = sums
        for i in range(4):
            saved[i, k] = sums[i]
        silu_val, first, _ = silu_parts(gate)
        return (
            (silu_val * upper).astype(BF16),
            (first * gate_dot * upper + silu_val * upper_dot).astype(BF16),
        )

    def consume_up(k):
        weights = down.take(k)
        half, columns = lax.div(k, z.steps), span(lax.rem(k, z.steps), z.chunk)
        hidden, hidden_dot = hid[half_rows(k), columns], hid_dot[half_rows(k), columns]
        totals[half, 0] += matmul(hidden, weights[0])
        totals[half, 1] += matmul(hidden_dot, weights[0]) + matmul(hidden, weights[1])

    def produce_back(k, part, slot):
        weights = again.take(k)
        grad, grad_dot = grads[0, half_rows(k), :], grads[1, half_rows(k), :]
        part[0, slot] = tail_dot(grad, weights[0])
        part[1, slot] = tail_dot(grad_dot, weights[0]) + tail_dot(grad, weights[1])

    def combine_back(k, sums):
        back, back_dot = sums
        gate, gate_dot, upper, upper_dot = [saved[i, k] for i in range(4)]
        silu_val, first, second = silu_parts(gate)
        return (
            (
                back_dot * upper * first + back * upper_dot * first + back * upper * second * gate_dot
            ).astype(BF16),
            (back_dot * silu_val + back * first * gate_dot).astype(BF16),
        )

    forward.bind(f_refs, hid, hid_dot, produce_up, combine_up, consume_up)
    backward.bind(b_refs, gate_in, upper_in, produce_back, combine_back, None)

    barrier = pltpu.get_barrier_semaphore()

    def greet(axis, peer):
        pl.semaphore_signal(
            barrier, inc=1, device_id={axis: peer}, device_id_type=pl.DeviceIdType.MESH
        )

    greet("gx", forward.partner)
    pl.when(forward.spot > 0)(lambda: greet("gx", forward.me - 2))
    pl.when(forward.spot < forward.last)(lambda: greet("gx", forward.me + 2))
    for peer in [other, *peers]:
        greet("gy", peer)
    up.start(0)
    down.start(0)
    again.start(0)
    totals[...] = jnp.zeros_like(totals)
    pl.semaphore_wait(barrier, z.pairs + jnp.where(forward.at_end, 2, 3))

    def x_rows(h, index):
        return x_full.at[span(h * z.gy + index, z.own)]

    def x_copy(h, s):
        return remote(tokens.at[span(h, z.own)], x_rows(h, me), x1, (h, s), "gy", peers[s])

    def x_side(h):
        return remote(tokens.at[span(h, z.own)], x_rows(h, me), x2, h, "gy", other)

    def x_pass(h, s):
        block = x_rows(h, sources[s])
        return remote(block, block, x3, (h, s), "gy", other)

    for h in range(z.halves):
        for s in hops:
            x_copy(h, s).start()
        x_side(h).start()
        x_rows(h, me)[...] = tokens[h * z.own : (h + 1) * z.own, :]
    for h in range(z.halves):
        for s in hops:
            x_copy(h, s).wait_recv()
            x_pass(h, s).start()
    for h in range(z.halves):
        x_side(h).wait_recv()
        for s in hops:
            x_pass(h, s).wait_recv()

    def own_rows(index):
        return span(index, z.own)

    def m1_copy(h):
        return remote(m1_out.at[h], m1_in.at[h], m1, h, "gy", other)

    def m2_copy(h, s):
        return remote(m2_out.at[h, s], m2_in.at[h, s], m2, (h, s), "gy", peers[s])

    def grad_rows(h, index):
        return grads.at[:, span(h * z.gy + index, z.own), :]

    def m3_copy(h, s):
        return remote(grad_rows(h, me), grad_rows(h, me), m3, (h, s), "gy", peers[s])

    def m3_side(h):
        return remote(grad_rows(h, me), grad_rows(h, me), m3p, h, "gy", other)

    def m4_copy(h, s):
        block = grad_rows(h, sources[s])
        return remote(block, block, m4, (h, s), "gy", other)

    ready = z.steps - 1 + 2 * z.line
    start_back = ready + 4

    def middle_send(t):
        for h in range(z.halves):

            @pl.when(t == ready + h * z.steps)
            def _():
                for i in (0, 1):
                    for g in range(z.pairs):
                        m1_out[h, i, g] = totals[h, i, own_rows(g * 2 + 1 - core), :].astype(BF16)
                m1_copy(h).start()

    def middle(t):
        for h in range(z.halves):
            base = ready + h * z.steps

            @pl.when(t == base + 1)
            def _():
                m1_copy(h).wait_recv()
                for i in (0, 1):
                    totals[h, i, own_rows(me), :] += m1_in[h, i, pair].astype(F32)
                for s in hops:
                    g = lax.div(peers[s], 2)
                    for i in (0, 1):
                        m2_out[h, s, i] = (
                            totals[h, i, own_rows(peers[s]), :] + m1_in[h, i, g].astype(F32)
                        ).astype(BF16)
                    m2_copy(h, s).start()

            @pl.when(t == base + 2)
            def _():
                outs = [totals[h, i, own_rows(me), :] for i in (0, 1)]
                for s in hops:
                    m2_copy(h, s).wait_recv()
                    outs = [outs[i] + m2_in[h, s, i].astype(F32) for i in (0, 1)]
                goal = target[h * z.own : (h + 1) * z.own, :].astype(F32)
                grad_rows(h, me)[0] = ((outs[0] - goal) * scale).astype(BF16)
                grad_rows(h, me)[1] = (outs[1] * scale).astype(BF16)
                for s in hops:
                    m3_copy(h, s).start()
                m3_side(h).start()

            @pl.when(t == base + 3)
            def _():
                for s in hops:
                    m3_copy(h, s).wait_recv()
                    m4_copy(h, s).start()

            @pl.when(t == base + 4)
            def _():
                m3_side(h).wait_recv()
                for s in hops:
                    m4_copy(h, s).wait_recv()

    def step(t, carry):
        forward.early(t)
        middle(t)
        backward.early(t - start_back)
        forward.late(t)
        middle_send(t)
        backward.late(t - start_back)
        return carry

    lax.fori_loop(0, start_back + z.items + 2 * z.line, step, 0)

    for h in range(z.halves):
        for s in hops:
            x_copy(h, s).wait_send()
            x_pass(h, s).wait_send()
            m2_copy(h, s).wait_send()
            m3_copy(h, s).wait_send()
            m4_copy(h, s).wait_send()
        x_side(h).wait_send()
        m1_copy(h).wait_send()
        m3_side(h).wait_send()

    def settle(k, carry):
        forward.settle(k)
        backward.settle(k)
        return carry

    lax.fori_loop(0, z.items, settle, 0)


def run(tokens, target, w_gate, w_up, w_down, t_gate, t_up, t_down):
    z = Sizes(tokens, w_gate)
    model = w_down.shape[1]
    tall = z.halves * z.rows
    forward, backward = Stream(z, 2, 2), Stream(z, 1, 1)
    vmem, any_spec = pl.BlockSpec(memory_space=pltpu.VMEM), pl.BlockSpec(memory_space=pl.ANY)
    sem = pltpu.SemaphoreType.DMA
    hops = max(z.pairs - 1, 1)
    wide = jax.ShapeDtypeStruct((tall, z.width), BF16)
    marks = [(z.halves, hops), (z.halves,), (z.halves, hops), (z.halves,), (z.halves, hops),
             (z.halves, hops), (z.halves,), (z.halves, hops)]
    return pl.pallas_call(
        functools.partial(hvp_kernel, z, 1.0 / math.sqrt(TOKENS), forward, backward),
        out_shape=[
            jax.ShapeDtypeStruct((tall, z.depth), BF16),
            wide,
            wide,
            jax.ShapeDtypeStruct((2, tall, model), BF16),
            wide,
            wide,
        ],
        in_specs=[vmem] * 2 + [any_spec] * 6,
        out_specs=[vmem] * 6,
        scratch_shapes=[
            *forward.scratch(),
            *backward.scratch(),
            pltpu.VMEM((2, 4, z.depth, z.chunk), BF16),
            sem((2, 4)),
            pltpu.VMEM((2, 2, z.chunk, model), BF16),
            sem((2, 2)),
            pltpu.VMEM((2, 2, z.chunk, model), BF16),
            sem((2, 2)),
            pltpu.VMEM((z.halves, 2, z.rows, model), F32),
            pltpu.VMEM((4, z.items, z.group, z.chunk), F32),
            pltpu.VMEM((z.halves, 2, z.pairs, z.own, model), BF16),
            pltpu.VMEM((z.halves, 2, z.pairs, z.own, model), BF16),
            pltpu.VMEM((z.halves, hops, 2, z.own, model), BF16),
            pltpu.VMEM((z.halves, hops, 2, z.own, model), BF16),
            *[sem(shape) for shape in marks for _ in range(2)],
        ],
        compiler_params=pltpu.CompilerParams(
            collective_id=0, has_side_effects=True, vmem_limit_bytes=67043328
        ),
        cost_estimate=pl.CostEstimate(
            flops=20 * tall * z.depth * z.width,
            bytes_accessed=60 * tall * z.width,
            transcendentals=0,
        ),
    )(tokens, target, w_gate, w_up, t_gate, t_up, w_down, t_down)


def products_kernel(turned, gate, upper, hidden, hidden_dot, grads, out_gate, out_up, out_down):
    out_gate[...] = matmul(turned[...], gate[...]).astype(BF16)
    out_up[...] = matmul(turned[...], upper[...]).astype(BF16)
    out_down[...] = (
        lead_dot(hidden_dot[...], grads[0]) + lead_dot(hidden[...], grads[1])
    ).astype(BF16)


def weight_products(turned, gate, upper, hidden, hidden_dot, grads):
    depth, rows = turned.shape
    width, model = gate.shape[1], grads.shape[2]
    tile = next(size for size in CHUNKS if width % size == 0)
    strip = pl.BlockSpec((rows, tile), lambda i: (0, i))
    return pl.pallas_call(
        products_kernel,
        grid=(width // tile,),
        in_specs=[
            pl.BlockSpec((depth, rows), lambda i: (0, 0)),
            *[strip] * 4,
            pl.BlockSpec((2, rows, model), lambda i: (0, 0, 0)),
        ],
        out_specs=[
            pl.BlockSpec((depth, tile), lambda i: (0, i)),
            pl.BlockSpec((depth, tile), lambda i: (0, i)),
            pl.BlockSpec((tile, model), lambda i: (i, 0)),
        ],
        out_shape=[
            jax.ShapeDtypeStruct((depth, width), BF16),
            jax.ShapeDtypeStruct((depth, width), BF16),
            jax.ShapeDtypeStruct((width, model), BF16),
        ],
        cost_estimate=pl.CostEstimate(
            flops=4 * rows * (depth + model) * width,
            bytes_accessed=2 * (2 * depth + model + 4 * rows) * width,
            transcendentals=0,
        ),
    )(turned, gate, upper, hidden, hidden_dot, grads)


def body(tokens, target, w_gate, w_up, w_down, t_gate, t_up, t_down):
    x_full, hidden, hidden_dot, grads, gate_in, upper_in = run(
        tokens, target, w_gate, w_up, w_down, t_gate, t_up, t_down
    )
    turned = lax.optimization_barrier(x_full.T)
    return tuple(weight_products(turned, gate_in, upper_in, hidden, hidden_dot, grads))


def solution(mesh):
    return jax.shard_map(
        body,
        mesh=mesh,
        in_specs=(
            P("gy", "gx"),
            P("gy", "gx"),
            P("gx", "gy"),
            P("gx", "gy"),
            P("gy", "gx"),
            P("gx", "gy"),
            P("gx", "gy"),
            P("gy", "gx"),
        ),
        out_specs=(P("gx", "gy"), P("gx", "gy"), P("gy", "gx")),
        check_vma=False,
    )
```

```python
import functools
import math

import jax
import jax.numpy as jnp
from jax import lax
from jax.experimental import pallas as pl
from jax.experimental.pallas import tpu as pltpu
from jax.sharding import PartitionSpec as P

TOKENS = 256
CHUNKS = (256, 128)
TILES = (896, 512, 256, 128)
LAG_UP, LAG_MIDDLE, LAG_BACK = 2, 2, 3
F32, BF16 = jnp.float32, jnp.bfloat16


def silu_parts(gate):
    sig = jax.nn.sigmoid(gate)
    first = sig * (1.0 + gate * (1.0 - sig))
    second = sig * (1.0 - sig) * (2.0 + gate * (1.0 - 2.0 * sig))
    return (gate * sig, first, second)


def matmul(left, right):
    return jnp.dot(left, right, preferred_element_type=F32)


def lead_dot(left, right):
    return lax.dot_general(left, right, (((0,), (0,)), ((), ())), preferred_element_type=F32)


def tail_dot(left, right):
    return lax.dot_general(left, right, (((1,), (1,)), ((), ())), preferred_element_type=F32)


def between(value, low, high):
    return jnp.logical_and(value >= low, value < high)


def both(*terms):
    return functools.reduce(jnp.logical_and, terms)


def span(start, size):
    return pl.ds(pl.multiple_of(start * size, size), size)


def remote(src, dst, sems, index, axis, peer):
    return pltpu.make_async_remote_copy(
        src_ref=src,
        dst_ref=dst,
        send_sem=sems[0].at[index],
        recv_sem=sems[1].at[index],
        device_id={axis: peer},
        device_id_type=pl.DeviceIdType.MESH,
    )


class Sizes:
    def __init__(self, tokens, w_gate):
        self.line = lax.axis_size("gx") // 2
        self.gy = lax.axis_size("gy")
        self.pairs = self.gy // 2
        own, self.depth = tokens.shape
        self.width = w_gate.shape[1]
        self.halves = 2 if own % 32 == 0 else 1
        self.own = own // self.halves
        self.rows = self.own * self.gy
        self.group = self.rows // 4
        self.chunk = next(size for size in CHUNKS if self.width % size == 0)
        self.steps = self.width // self.chunk
        self.items = self.halves * self.steps


class Stream:
    def __init__(self, sizes, na, nb, lag):
        self.z, self.na, self.nb, self.lag = sizes, na, nb, lag

    def scratch(self):
        z, na, nb = self.z, self.na, self.nb
        n, g, c = z.items, z.group, z.chunk
        sem = pltpu.SemaphoreType.DMA
        pairs = [(n,), (2, n), (2, n), (n,), (2, n), (2, n), (n,), (2, n)]
        return [
            pltpu.VMEM((na + nb, self.lag * z.line, z.rows, c), F32),
            pltpu.VMEM((n, na, 2, g, c), BF16),
            pltpu.VMEM((n, na, 2, g, c), BF16),
            pltpu.VMEM((2, n, na, g, c), BF16),
            pltpu.VMEM((2, n, nb, 2 * g, c), BF16),
            pltpu.VMEM((n, nb, g, c), BF16),
            pltpu.VMEM((n, nb, g, c), BF16),
            *[sem(shape) for shape in pairs for _ in range(2)],
        ]

    def bind(self, refs, full0, full1, produce, combine, consume):
        self.part, self.y_out, self.y_in, self.a, self.b, self.f_out, self.f_in = refs[:7]
        sems = [(refs[7 + 2 * i], refs[8 + 2 * i]) for i in range(8)]
        (self.ys, self.as_, self.bs, self.fs, self.hs, self.gs, self.xs, self.ks) = sems
        self.full0, self.full1 = full0, full1
        self.produce, self.combine, self.consume = produce, combine, consume
        z = self.z
        self.me = lax.axis_index("gx")
        self.spot, self.side = lax.div(self.me, 2), lax.rem(self.me, 2)
        self.partner = self.me + 1 - 2 * self.side
        self.last = z.line - 1
        self.at_end = jnp.logical_or(self.spot == 0, self.spot == self.last)
        self.end = jnp.where(self.spot == 0, 0, 1)
        self.place = [self.last - self.spot, self.spot]

    def group_of(self, e, s):
        return span(e * 2 + s, self.z.group)

    def block(self, full, k, e, s):
        z = self.z
        half, j = lax.div(k, z.steps), lax.rem(k, z.steps)
        return full.at[span(half * 4 + e * 2 + s, z.group), span(j, z.chunk)]

    def slab(self, full, k, e):
        z = self.z
        half, j = lax.div(k, z.steps), lax.rem(k, z.steps)
        return full.at[span(half * 2 + e, 2 * z.group), span(j, z.chunk)]

    def across(self, src, dst, sems, index):
        return remote(src, dst, sems, index, "gx", self.partner)

    def along(self, d, src, dst, sems, index):
        return remote(src, dst, sems, index, "gx", self.me - 2 + 4 * d)

    def y_copy(self, k):
        return self.across(self.y_out.at[k], self.y_in.at[k], self.ys, k)

    def f_copy(self, k):
        return self.across(self.f_out.at[k], self.f_in.at[k], self.fs, k)

    def a_copy(self, d, k):
        return self.along(d, self.a.at[d, k], self.a.at[d, k], self.as_, (d, k))

    def b_copy(self, d, k):
        return self.along(d, self.b.at[d, k], self.b.at[d, k], self.bs, (d, k))

    def h_copy(self, d, k):
        block = self.block(self.full0, k, 1 - d, self.side)
        return self.along(d, block, block, self.hs, (d, k))

    def g_copy(self, d, k):
        block = self.block(self.full0, k, 1 - d, self.side)
        return self.across(block, block, self.gs, (d, k))

    def x_copy(self, k):
        block = self.block(self.full1, k, self.end, self.side)
        return self.across(block, block, self.xs, k)

    def k_copy(self, d, k):
        block = self.slab(self.full1, k, 1 - d)
        return self.along(d, block, block, self.ks, (d, k))

    def early(self, t):
        z, last, side, na, nb = self.z, self.last, self.side, self.na, self.nb
        n, part, a, b = z.items, self.part, self.a, self.b
        for d in (0, 1):
            p = self.place[d]
            k, h = t - self.lag * (z.line + 1 + p), t - self.lag * (z.line + p)
            go = between(k, 0, n)

            @pl.when(both(go, p > 0))
            def _():
                self.k_copy(d, k).wait_recv()

            @pl.when(both(go, p == 0))
            def _():
                self.x_copy(k).wait_recv()

            @pl.when(both(go, p < last))
            def _():
                self.k_copy(d, k).start()

            @pl.when(both(between(h, 0, n), p > 0))
            def _():
                self.h_copy(d, h).wait_recv()
                self.g_copy(d, h).start()

            @pl.when(both(between(h, 0, n), between(p, 1, last)))
            def _():
                self.h_copy(d, h).start()

            @pl.when(go)
            def _():
                self.g_copy(d, k).wait_recv()

        k = t - self.lag * z.line

        @pl.when(both(between(k, 0, n), self.at_end))
        def _():
            self.a_copy(self.end, k).wait_recv()
            self.f_copy(k).wait_recv()
            slot, mine = lax.rem(k, self.lag * z.line), self.group_of(self.end, side)
            sums = [part[i, slot, mine, :] + a[self.end, k, i].astype(F32) for i in range(na)]
            sums += [part[na + i, slot, mine, :] + self.f_in[k, i].astype(F32) for i in range(nb)]
            first, second = self.combine(k, sums)
            self.block(self.full0, k, self.end, side)[...] = first
            self.block(self.full1, k, self.end, side)[...] = second
            self.x_copy(k).start()
            self.h_copy(1 - self.end, k).start()
            self.g_copy(1 - self.end, k).start()

        for d in (0, 1):
            p = self.place[d]
            k = t - self.lag * p

            @pl.when(both(between(k, 0, n), between(p, 1, last)))
            def _():
                self.b_copy(d, k).wait_recv()
                slot, slab = lax.rem(k, self.lag * z.line), span(d, 2 * z.group)
                for i in range(nb):
                    b[d, k, i] = (part[na + i, slot, slab, :] + b[d, k, i].astype(F32)).astype(BF16)
                self.b_copy(d, k).start()

            @pl.when(both(between(k, 0, n), p == last))
            def _():
                self.b_copy(d, k).wait_recv()
                slot = lax.rem(k, self.lag * z.line)
                own, other = span(side, z.group), span(1 - side, z.group)
                for i in range(nb):
                    self.f_out[k, i] = (
                        part[na + i, slot, self.group_of(d, 1 - side), :]
                        + b[d, k, i, other, :].astype(F32)
                    ).astype(BF16)
                self.f_copy(k).start()
                for i in range(nb):
                    part[na + i, slot, self.group_of(d, side), :] += b[d, k, i, own, :].astype(F32)

        k = t - self.lag

        @pl.when(between(k, 0, n))
        def _():
            self.y_copy(k).wait_recv()
            for i in range(na):
                for e in (0, 1):
                    part[i, lax.rem(k, self.lag * z.line), self.group_of(e, side), :] += self.y_in[
                        k, i, e
                    ].astype(F32)

        for d in (0, 1):
            p = self.place[d]
            k = t - self.lag * (1 + p)

            @pl.when(both(between(k, 0, n), between(p, 1, last)))
            def _():
                self.a_copy(d, k).wait_recv()
                for i in range(na):
                    a[d, k, i] = (
                        part[i, lax.rem(k, self.lag * z.line), self.group_of(d, side), :]
                        + a[d, k, i].astype(F32)
                    ).astype(BF16)
                self.a_copy(d, k).start()

            @pl.when(both(between(k, 0, n), p == 0))
            def _():
                for i in range(na):
                    a[d, k, i] = part[i, lax.rem(k, self.lag * z.line), self.group_of(d, side), :].astype(BF16)
                self.a_copy(d, k).start()

    def late(self, t):
        z, na, nb = self.z, self.na, self.nb

        @pl.when(between(t, 0, z.items))
        def _():
            slot = lax.rem(t, self.lag * z.line)
            self.produce(t, self.part, slot)
            for i in range(na):
                for e in (0, 1):
                    self.y_out[t, i, e] = self.part[
                        i, slot, self.group_of(e, 1 - self.side), :
                    ].astype(BF16)
            self.y_copy(t).start()

            @pl.when(self.at_end)
            def _():
                d = 1 - self.end
                for i in range(nb):
                    self.b[d, t, i] = self.part[na + i, slot, span(d, 2 * z.group), :].astype(BF16)
                self.b_copy(d, t).start()

        if self.consume is not None:
            k = t - 2 * self.lag * z.line

            @pl.when(between(k, 0, z.items))
            def _():
                self.consume(k)

    def settle(self, k):
        self.y_copy(k).wait_send()

        @pl.when(self.at_end)
        def _():
            self.f_copy(k).wait_send()
            self.x_copy(k).wait_send()

        for d in (0, 1):
            self.g_copy(d, k).wait_send()

            @pl.when(self.place[d] < self.last)
            def _():
                self.a_copy(d, k).wait_send()
                self.b_copy(d, k).wait_send()
                self.h_copy(d, k).wait_send()
                self.k_copy(d, k).wait_send()


class Feed:
    def __init__(self, sources, slots, sems, sizes, view):
        self.sources, self.slots, self.sems = sources, slots, sems
        self.sizes, self.view = sizes, view

    def copies(self, k):
        slot, j = lax.rem(k, 2), lax.rem(k, self.sizes.steps)
        return [
            pltpu.make_async_copy(
                self.view(source, j), self.slots.at[slot, i], self.sems.at[slot, i]
            )
            for i, source in enumerate(self.sources)
        ]

    def start(self, k):
        for copy in self.copies(k):
            copy.start()

    def take(self, k):
        for copy in self.copies(k):
            copy.wait()
        pl.when(k + 1 < self.sizes.items)(lambda: self.start(k + 1))
        return self.slots.at[lax.rem(k, 2)]


def hvp_kernel(z, scale, forward, backward, *refs):
    tokens, target, w_gate, w_up, t_gate, t_up, w_down, t_down = refs[:8]
    x_full, hid, hid_dot, grads, gate_in, upper_in = refs[8:14]
    count = len(forward.scratch())
    f_refs, b_refs, rest = refs[14 : 14 + count], refs[14 + count : 14 + 2 * count], refs[14 + 2 * count :]
    up_slots, up_sems, down_slots, down_sems, back_slots, back_sems = rest[:6]
    totals, saved, m1_out, m1_in, m2_out, m2_in = rest[6:12]
    sems = [(rest[12 + 2 * i], rest[13 + 2 * i]) for i in range(8)]
    x1, x2, x3, m1, m2, m3, m3p, m4 = sems

    me = lax.axis_index("gy")
    core, pair = lax.rem(me, 2), lax.div(me, 2)
    other = me + 1 - 2 * core
    peers = [lax.rem(pair + s, z.pairs) * 2 + core for s in range(1, z.pairs)]
    sources = [lax.rem(pair + z.pairs - s, z.pairs) * 2 + core for s in range(1, z.pairs)]
    hops = range(z.pairs - 1)

    up = Feed((w_gate, w_up, t_gate, t_up), up_slots, up_sems, z, lambda r, j: r.at[:, span(j, z.chunk)])
    down = Feed((w_down, t_down), down_slots, down_sems, z, lambda r, j: r.at[span(j, z.chunk), :])
    again = Feed((w_down, t_down), back_slots, back_sems, z, lambda r, j: r.at[span(j, z.chunk), :])

    def half_rows(k):
        return span(lax.div(k, z.steps), z.rows)

    def produce_up(k, part, slot):
        weights = up.take(k)
        x = x_full[half_rows(k), :]
        for i in range(4):
            part[i, slot] = matmul(x, weights[(0, 2, 1, 3)[i]])

    def combine_up(k, sums):
        gate, gate_dot, upper, upper_dot = sums
        for i in range(4):
            saved[i, k] = sums[i]
        silu_val, first, _ = silu_parts(gate)
        return (
            (silu_val * upper).astype(BF16),
            (first * gate_dot * upper + silu_val * upper_dot).astype(BF16),
        )

    def consume_up(k):
        weights = down.take(k)
        half, columns = lax.div(k, z.steps), span(lax.rem(k, z.steps), z.chunk)
        hidden, hidden_dot = hid[half_rows(k), columns], hid_dot[half_rows(k), columns]
        totals[half, 0] += matmul(hidden, weights[0])
        totals[half, 1] += matmul(hidden_dot, weights[0]) + matmul(hidden, weights[1])

    def produce_back(k, part, slot):
        weights = again.take(k)
        grad, grad_dot = grads[0, half_rows(k), :], grads[1, half_rows(k), :]
        part[0, slot] = tail_dot(grad, weights[0])
        part[1, slot] = tail_dot(grad_dot, weights[0]) + tail_dot(grad, weights[1])

    def combine_back(k, sums):
        back, back_dot = sums
        gate, gate_dot, upper, upper_dot = [saved[i, k] for i in range(4)]
        silu_val, first, second = silu_parts(gate)
        return (
            (
                back_dot * upper * first + back * upper_dot * first + back * upper * second * gate_dot
            ).astype(BF16),
            (back_dot * silu_val + back * first * gate_dot).astype(BF16),
        )

    forward.bind(f_refs, hid, hid_dot, produce_up, combine_up, consume_up)
    backward.bind(b_refs, gate_in, upper_in, produce_back, combine_back, None)

    barrier = pltpu.get_barrier_semaphore()

    def greet(axis, peer):
        pl.semaphore_signal(
            barrier, inc=1, device_id={axis: peer}, device_id_type=pl.DeviceIdType.MESH
        )

    greet("gx", forward.partner)
    pl.when(forward.spot > 0)(lambda: greet("gx", forward.me - 2))
    pl.when(forward.spot < forward.last)(lambda: greet("gx", forward.me + 2))
    for peer in [other, *peers]:
        greet("gy", peer)
    up.start(0)
    down.start(0)
    again.start(0)
    totals[...] = jnp.zeros_like(totals)
    pl.semaphore_wait(barrier, z.pairs + jnp.where(forward.at_end, 2, 3))

    def x_rows(h, index):
        return x_full.at[span(h * z.gy + index, z.own)]

    def x_copy(h, s):
        return remote(tokens.at[span(h, z.own)], x_rows(h, me), x1, (h, s), "gy", peers[s])

    def x_side(h):
        return remote(tokens.at[span(h, z.own)], x_rows(h, me), x2, h, "gy", other)

    def x_pass(h, s):
        block = x_rows(h, sources[s])
        return remote(block, block, x3, (h, s), "gy", other)

    for h in range(z.halves):
        for s in hops:
            x_copy(h, s).start()
        x_side(h).start()
        x_rows(h, me)[...] = tokens[h * z.own : (h + 1) * z.own, :]

    def x_relay(h):
        for s in hops:
            x_copy(h, s).wait_recv()
            x_pass(h, s).start()

    def x_take(h):
        x_side(h).wait_recv()
        for s in hops:
            x_pass(h, s).wait_recv()

    x_relay(0)
    x_take(0)

    def own_rows(index):
        return span(index, z.own)

    def m1_copy(h):
        return remote(m1_out.at[h], m1_in.at[h], m1, h, "gy", other)

    def m2_copy(h, s):
        return remote(m2_out.at[h, s], m2_in.at[h, s], m2, (h, s), "gy", peers[s])

    def grad_rows(h, index):
        return grads.at[:, span(h * z.gy + index, z.own), :]

    def m3_copy(h, s):
        return remote(grad_rows(h, me), grad_rows(h, me), m3, (h, s), "gy", peers[s])

    def m3_side(h):
        return remote(grad_rows(h, me), grad_rows(h, me), m3p, h, "gy", other)

    def m4_copy(h, s):
        block = grad_rows(h, sources[s])
        return remote(block, block, m4, (h, s), "gy", other)

    ready = z.steps - 1 + 2 * LAG_UP * z.line
    start_back = ready + 3 * LAG_MIDDLE

    def middle_send(t):
        for h in range(z.halves):

            @pl.when(t == ready + h * z.steps)
            def _():
                for i in (0, 1):
                    for g in range(z.pairs):
                        m1_out[h, i, g] = totals[h, i, own_rows(g * 2 + 1 - core), :].astype(BF16)
                m1_copy(h).start()

    def middle(t):
        for h in range(z.halves):
            base = ready + h * z.steps

            @pl.when(t == base + LAG_MIDDLE)
            def _():
                m1_copy(h).wait_recv()
                for i in (0, 1):
                    totals[h, i, own_rows(me), :] += m1_in[h, i, pair].astype(F32)
                for s in hops:
                    g = lax.div(peers[s], 2)
                    for i in (0, 1):
                        m2_out[h, s, i] = (
                            totals[h, i, own_rows(peers[s]), :] + m1_in[h, i, g].astype(F32)
                        ).astype(BF16)
                    m2_copy(h, s).start()

            @pl.when(t == base + 2 * LAG_MIDDLE)
            def _():
                outs = [totals[h, i, own_rows(me), :] for i in (0, 1)]
                for s in hops:
                    m2_copy(h, s).wait_recv()
                    outs = [outs[i] + m2_in[h, s, i].astype(F32) for i in (0, 1)]
                goal = target[h * z.own : (h + 1) * z.own, :].astype(F32)
                grad_rows(h, me)[0] = ((outs[0] - goal) * scale).astype(BF16)
                grad_rows(h, me)[1] = (outs[1] * scale).astype(BF16)
                for s in hops:
                    m3_copy(h, s).start()
                m3_side(h).start()

            @pl.when(t == base + 3 * LAG_MIDDLE)
            def _():
                for s in hops:
                    m3_copy(h, s).wait_recv()
                    m4_copy(h, s).start()

    def middle_take(t):
        for h in range(z.halves):

            @pl.when(t == ready + h * z.steps + 3 * LAG_MIDDLE)
            def _():
                m3_side(h).wait_recv()
                for s in hops:
                    m4_copy(h, s).wait_recv()

    def x_later(t):
        for h in range(1, z.halves):
            pl.when(t == 1)(lambda: x_relay(h))
            pl.when(t == 3)(lambda: x_take(h))

    def step(t, carry):
        x_later(t)
        forward.early(t)
        middle(t)
        backward.early(t - start_back)
        forward.late(t)
        middle_send(t)
        middle_take(t)
        backward.late(t - start_back)
        return carry

    lax.fori_loop(0, start_back + z.items + 2 * LAG_BACK * z.line, step, 0)

    for h in range(z.halves):
        for s in hops:
            x_copy(h, s).wait_send()
            x_pass(h, s).wait_send()
            m2_copy(h, s).wait_send()
            m3_copy(h, s).wait_send()
            m4_copy(h, s).wait_send()
        x_side(h).wait_send()
        m1_copy(h).wait_send()
        m3_side(h).wait_send()

    def settle(k, carry):
        forward.settle(k)
        backward.settle(k)
        return carry

    lax.fori_loop(0, z.items, settle, 0)


def run(tokens, target, w_gate, w_up, w_down, t_gate, t_up, t_down):
    z = Sizes(tokens, w_gate)
    model = w_down.shape[1]
    tall = z.halves * z.rows
    forward, backward = Stream(z, 2, 2, LAG_UP), Stream(z, 1, 1, LAG_BACK)
    vmem, any_spec = pl.BlockSpec(memory_space=pltpu.VMEM), pl.BlockSpec(memory_space=pl.ANY)
    sem = pltpu.SemaphoreType.DMA
    hops = max(z.pairs - 1, 1)
    wide = jax.ShapeDtypeStruct((tall, z.width), BF16)
    marks = [(z.halves, hops), (z.halves,), (z.halves, hops), (z.halves,), (z.halves, hops),
             (z.halves, hops), (z.halves,), (z.halves, hops)]
    return pl.pallas_call(
        functools.partial(hvp_kernel, z, 1.0 / math.sqrt(TOKENS), forward, backward),
        out_shape=[
            jax.ShapeDtypeStruct((tall, z.depth), BF16),
            wide,
            wide,
            jax.ShapeDtypeStruct((2, tall, model), BF16),
            wide,
            wide,
        ],
        in_specs=[vmem] * 2 + [any_spec] * 6,
        out_specs=[vmem] * 6,
        scratch_shapes=[
            *forward.scratch(),
            *backward.scratch(),
            pltpu.VMEM((2, 4, z.depth, z.chunk), BF16),
            sem((2, 4)),
            pltpu.VMEM((2, 2, z.chunk, model), BF16),
            sem((2, 2)),
            pltpu.VMEM((2, 2, z.chunk, model), BF16),
            sem((2, 2)),
            pltpu.VMEM((z.halves, 2, z.rows, model), F32),
            pltpu.VMEM((4, z.items, z.group, z.chunk), F32),
            pltpu.VMEM((z.halves, 2, z.pairs, z.own, model), BF16),
            pltpu.VMEM((z.halves, 2, z.pairs, z.own, model), BF16),
            pltpu.VMEM((z.halves, hops, 2, z.own, model), BF16),
            pltpu.VMEM((z.halves, hops, 2, z.own, model), BF16),
            *[sem(shape) for shape in marks for _ in range(2)],
        ],
        compiler_params=pltpu.CompilerParams(
            collective_id=0, has_side_effects=True, vmem_limit_bytes=67043328
        ),
        cost_estimate=pl.CostEstimate(
            flops=20 * tall * z.depth * z.width,
            bytes_accessed=60 * tall * z.width,
            transcendentals=0,
        ),
    )(tokens, target, w_gate, w_up, t_gate, t_up, w_down, t_down)


def products_kernel(tokens, gate, upper, hidden, hidden_dot, grads, out_gate, out_up, out_down):
    out_gate[...] = lead_dot(tokens[...], gate[...]).astype(BF16)
    out_up[...] = lead_dot(tokens[...], upper[...]).astype(BF16)
    out_down[...] = (
        lead_dot(hidden_dot[...], grads[0]) + lead_dot(hidden[...], grads[1])
    ).astype(BF16)


def weight_products(tokens, gate, upper, hidden, hidden_dot, grads):
    rows, depth = tokens.shape
    width, model = gate.shape[1], grads.shape[2]
    tile = next(size for size in TILES if width % size == 0)
    strip = pl.BlockSpec((rows, tile), lambda i: (0, i))
    return pl.pallas_call(
        products_kernel,
        grid=(width // tile,),
        in_specs=[
            pl.BlockSpec((rows, depth), lambda i: (0, 0)),
            *[strip] * 4,
            pl.BlockSpec((2, rows, model), lambda i: (0, 0, 0)),
        ],
        out_specs=[
            pl.BlockSpec((depth, tile), lambda i: (0, i)),
            pl.BlockSpec((depth, tile), lambda i: (0, i)),
            pl.BlockSpec((tile, model), lambda i: (i, 0)),
        ],
        out_shape=[
            jax.ShapeDtypeStruct((depth, width), BF16),
            jax.ShapeDtypeStruct((depth, width), BF16),
            jax.ShapeDtypeStruct((width, model), BF16),
        ],
        cost_estimate=pl.CostEstimate(
            flops=4 * rows * (depth + model) * width,
            bytes_accessed=2 * (2 * depth + model + 4 * rows) * width,
            transcendentals=0,
        ),
    )(tokens, gate, upper, hidden, hidden_dot, grads)


def body(tokens, target, w_gate, w_up, w_down, t_gate, t_up, t_down):
    x_full, hidden, hidden_dot, grads, gate_in, upper_in = run(
        tokens, target, w_gate, w_up, w_down, t_gate, t_up, t_down
    )
    return tuple(weight_products(x_full, gate_in, upper_in, hidden, hidden_dot, grads))


def solution(mesh):
    return jax.shard_map(
        body,
        mesh=mesh,
        in_specs=(
            P("gy", "gx"),
            P("gy", "gx"),
            P("gx", "gy"),
            P("gx", "gy"),
            P("gy", "gx"),
            P("gx", "gy"),
            P("gx", "gy"),
            P("gy", "gx"),
        ),
        out_specs=(P("gx", "gy"), P("gx", "gy"), P("gy", "gx")),
        check_vma=False,
    )
```

```python
import functools
import math

import jax
import jax.numpy as jnp
from jax import lax
from jax.experimental import pallas as pl
from jax.experimental.pallas import tpu as pltpu
from jax.sharding import PartitionSpec as P

TOKENS = 256
CHUNKS = (512, 256, 128)
TILES = (896, 512, 256, 128)
LAG_UP, LAG_BACK = 2, 3
MIDDLE = (1, 3, 5)
F32, BF16 = jnp.float32, jnp.bfloat16


def silu_parts(gate):
    sig = jax.nn.sigmoid(gate)
    first = sig * (1.0 + gate * (1.0 - sig))
    second = sig * (1.0 - sig) * (2.0 + gate * (1.0 - 2.0 * sig))
    return (gate * sig, first, second)


def matmul(left, right):
    return jnp.dot(left, right, preferred_element_type=F32)


def lead_dot(left, right):
    return lax.dot_general(left, right, (((0,), (0,)), ((), ())), preferred_element_type=F32)


def tail_dot(left, right):
    return lax.dot_general(left, right, (((1,), (1,)), ((), ())), preferred_element_type=F32)


def between(value, low, high):
    return jnp.logical_and(value >= low, value < high)


def both(*terms):
    return functools.reduce(jnp.logical_and, terms)


def span(start, size):
    return pl.ds(pl.multiple_of(start * size, size), size)


def remote(src, dst, sems, index, axis, peer):
    return pltpu.make_async_remote_copy(
        src_ref=src,
        dst_ref=dst,
        send_sem=sems[0].at[index],
        recv_sem=sems[1].at[index],
        device_id={axis: peer},
        device_id_type=pl.DeviceIdType.MESH,
    )


class Sizes:
    def __init__(self, tokens, w_gate):
        self.line = lax.axis_size("gx") // 2
        self.gy = lax.axis_size("gy")
        self.pairs = self.gy // 2
        own, self.depth = tokens.shape
        self.width = w_gate.shape[1]
        self.halves = next(parts for parts in (4, 2, 1) if own % (16 * parts) == 0)
        self.own = own // self.halves
        self.rows = self.own * self.gy
        self.group = self.rows // 4
        self.chunk = next(size for size in CHUNKS if self.width % size == 0)
        self.steps = self.width // self.chunk
        self.items = self.halves * self.steps


class Stream:
    def __init__(self, sizes, na, nb, lag):
        self.z, self.na, self.nb, self.lag = sizes, na, nb, lag

    def scratch(self):
        z, na, nb = self.z, self.na, self.nb
        n, g, c = z.items, z.group, z.chunk
        sem = pltpu.SemaphoreType.DMA
        pairs = [(n,), (2, n), (2, n), (n,), (2, n), (2, n), (n,), (2, n)]
        return [
            pltpu.VMEM((na + nb, self.lag * z.line, z.rows, c), F32),
            pltpu.VMEM((n, na, 2, g, c), BF16),
            pltpu.VMEM((n, na, 2, g, c), BF16),
            pltpu.VMEM((2, n, na, g, c), BF16),
            pltpu.VMEM((2, n, nb, 2 * g, c), BF16),
            pltpu.VMEM((n, nb, g, c), BF16),
            pltpu.VMEM((n, nb, g, c), BF16),
            *[sem(shape) for shape in pairs for _ in range(2)],
        ]

    def bind(self, refs, full0, full1, produce, combine, consume):
        self.part, self.y_out, self.y_in, self.a, self.b, self.f_out, self.f_in = refs[:7]
        sems = [(refs[7 + 2 * i], refs[8 + 2 * i]) for i in range(8)]
        (self.ys, self.as_, self.bs, self.fs, self.hs, self.gs, self.xs, self.ks) = sems
        self.full0, self.full1 = full0, full1
        self.produce, self.combine, self.consume = produce, combine, consume
        z = self.z
        self.me = lax.axis_index("gx")
        self.spot, self.side = lax.div(self.me, 2), lax.rem(self.me, 2)
        self.partner = self.me + 1 - 2 * self.side
        self.last = z.line - 1
        self.at_end = jnp.logical_or(self.spot == 0, self.spot == self.last)
        self.end = jnp.where(self.spot == 0, 0, 1)
        self.place = [self.last - self.spot, self.spot]

    def group_of(self, e, s):
        return span(e * 2 + s, self.z.group)

    def block(self, full, k, e, s):
        z = self.z
        half, j = lax.div(k, z.steps), lax.rem(k, z.steps)
        return full.at[span(half * 4 + e * 2 + s, z.group), span(j, z.chunk)]

    def slab(self, full, k, e):
        z = self.z
        half, j = lax.div(k, z.steps), lax.rem(k, z.steps)
        return full.at[span(half * 2 + e, 2 * z.group), span(j, z.chunk)]

    def across(self, src, dst, sems, index):
        return remote(src, dst, sems, index, "gx", self.partner)

    def along(self, d, src, dst, sems, index):
        return remote(src, dst, sems, index, "gx", self.me - 2 + 4 * d)

    def y_copy(self, k):
        return self.across(self.y_out.at[k], self.y_in.at[k], self.ys, k)

    def f_copy(self, k):
        return self.across(self.f_out.at[k], self.f_in.at[k], self.fs, k)

    def a_copy(self, d, k):
        return self.along(d, self.a.at[d, k], self.a.at[d, k], self.as_, (d, k))

    def b_copy(self, d, k):
        return self.along(d, self.b.at[d, k], self.b.at[d, k], self.bs, (d, k))

    def h_copy(self, d, k):
        block = self.block(self.full0, k, 1 - d, self.side)
        return self.along(d, block, block, self.hs, (d, k))

    def g_copy(self, d, k):
        block = self.block(self.full0, k, 1 - d, self.side)
        return self.across(block, block, self.gs, (d, k))

    def x_copy(self, k):
        block = self.block(self.full1, k, self.end, self.side)
        return self.across(block, block, self.xs, k)

    def k_copy(self, d, k):
        block = self.slab(self.full1, k, 1 - d)
        return self.along(d, block, block, self.ks, (d, k))

    def early(self, t):
        z, last, side, na, nb = self.z, self.last, self.side, self.na, self.nb
        n, part, a, b = z.items, self.part, self.a, self.b
        for d in (0, 1):
            p = self.place[d]
            k, h = t - self.lag * (z.line + 1 + p), t - self.lag * (z.line + p)
            go = between(k, 0, n)

            @pl.when(both(go, p > 0))
            def _():
                self.k_copy(d, k).wait_recv()

            @pl.when(both(go, p == 0))
            def _():
                self.x_copy(k).wait_recv()

            @pl.when(both(go, p < last))
            def _():
                self.k_copy(d, k).start()

            @pl.when(both(between(h, 0, n), p > 0))
            def _():
                self.h_copy(d, h).wait_recv()
                self.g_copy(d, h).start()

            @pl.when(both(between(h, 0, n), between(p, 1, last)))
            def _():
                self.h_copy(d, h).start()

            @pl.when(go)
            def _():
                self.g_copy(d, k).wait_recv()

        k = t - self.lag * z.line

        @pl.when(both(between(k, 0, n), self.at_end))
        def _():
            self.a_copy(self.end, k).wait_recv()
            self.f_copy(k).wait_recv()
            slot, mine = lax.rem(k, self.lag * z.line), self.group_of(self.end, side)
            sums = [part[i, slot, mine, :] + a[self.end, k, i].astype(F32) for i in range(na)]
            sums += [part[na + i, slot, mine, :] + self.f_in[k, i].astype(F32) for i in range(nb)]
            first, second = self.combine(k, sums)
            self.block(self.full0, k, self.end, side)[...] = first
            self.block(self.full1, k, self.end, side)[...] = second
            self.x_copy(k).start()
            self.h_copy(1 - self.end, k).start()
            self.g_copy(1 - self.end, k).start()

        for d in (0, 1):
            p = self.place[d]
            k = t - self.lag * p

            @pl.when(both(between(k, 0, n), between(p, 1, last)))
            def _():
                self.b_copy(d, k).wait_recv()
                slot, slab = lax.rem(k, self.lag * z.line), span(d, 2 * z.group)
                for i in range(nb):
                    b[d, k, i] = (part[na + i, slot, slab, :] + b[d, k, i].astype(F32)).astype(BF16)
                self.b_copy(d, k).start()

            @pl.when(both(between(k, 0, n), p == last))
            def _():
                self.b_copy(d, k).wait_recv()
                slot = lax.rem(k, self.lag * z.line)
                own, other = span(side, z.group), span(1 - side, z.group)
                for i in range(nb):
                    self.f_out[k, i] = (
                        part[na + i, slot, self.group_of(d, 1 - side), :]
                        + b[d, k, i, other, :].astype(F32)
                    ).astype(BF16)
                self.f_copy(k).start()
                for i in range(nb):
                    part[na + i, slot, self.group_of(d, side), :] += b[d, k, i, own, :].astype(F32)

        k = t - self.lag

        @pl.when(between(k, 0, n))
        def _():
            self.y_copy(k).wait_recv()
            for i in range(na):
                for e in (0, 1):
                    part[i, lax.rem(k, self.lag * z.line), self.group_of(e, side), :] += self.y_in[
                        k, i, e
                    ].astype(F32)

        for d in (0, 1):
            p = self.place[d]
            k = t - self.lag * (1 + p)

            @pl.when(both(between(k, 0, n), between(p, 1, last)))
            def _():
                self.a_copy(d, k).wait_recv()
                for i in range(na):
                    a[d, k, i] = (
                        part[i, lax.rem(k, self.lag * z.line), self.group_of(d, side), :]
                        + a[d, k, i].astype(F32)
                    ).astype(BF16)
                self.a_copy(d, k).start()

            @pl.when(both(between(k, 0, n), p == 0))
            def _():
                for i in range(na):
                    a[d, k, i] = part[i, lax.rem(k, self.lag * z.line), self.group_of(d, side), :].astype(BF16)
                self.a_copy(d, k).start()

    def late(self, t):
        z, na, nb = self.z, self.na, self.nb

        @pl.when(between(t, 0, z.items))
        def _():
            slot = lax.rem(t, self.lag * z.line)
            self.produce(t, self.part, slot)
            for i in range(na):
                for e in (0, 1):
                    self.y_out[t, i, e] = self.part[
                        i, slot, self.group_of(e, 1 - self.side), :
                    ].astype(BF16)
            self.y_copy(t).start()

            @pl.when(self.at_end)
            def _():
                d = 1 - self.end
                for i in range(nb):
                    self.b[d, t, i] = self.part[na + i, slot, span(d, 2 * z.group), :].astype(BF16)
                self.b_copy(d, t).start()

        if self.consume is not None:
            k = t - 2 * self.lag * z.line

            @pl.when(between(k, 0, z.items))
            def _():
                self.consume(k)

    def settle(self, k):
        self.y_copy(k).wait_send()

        @pl.when(self.at_end)
        def _():
            self.f_copy(k).wait_send()
            self.x_copy(k).wait_send()

        for d in (0, 1):
            self.g_copy(d, k).wait_send()

            @pl.when(self.place[d] < self.last)
            def _():
                self.a_copy(d, k).wait_send()
                self.b_copy(d, k).wait_send()
                self.h_copy(d, k).wait_send()
                self.k_copy(d, k).wait_send()


class Feed:
    def __init__(self, sources, slots, sems, sizes, view):
        self.sources, self.slots, self.sems = sources, slots, sems
        self.sizes, self.view = sizes, view

    def copies(self, k):
        slot, j = lax.rem(k, 2), lax.rem(k, self.sizes.steps)
        return [
            pltpu.make_async_copy(
                self.view(source, j), self.slots.at[slot, i], self.sems.at[slot, i]
            )
            for i, source in enumerate(self.sources)
        ]

    def start(self, k):
        for copy in self.copies(k):
            copy.start()

    def take(self, k):
        for copy in self.copies(k):
            copy.wait()
        pl.when(k + 1 < self.sizes.items)(lambda: self.start(k + 1))
        return self.slots.at[lax.rem(k, 2)]


def hvp_kernel(z, scale, forward, backward, *refs):
    tokens, target, w_gate, w_up, t_gate, t_up, w_down, t_down = refs[:8]
    results = refs[8:14]
    count = len(forward.scratch())
    f_refs, b_refs, rest = refs[14 : 14 + count], refs[14 + count : 14 + 2 * count], refs[14 + 2 * count :]
    up_slots, up_sems, down_slots, down_sems, back_slots, back_sems = rest[:6]
    totals, saved, m1_out, m1_in, m2_out, m2_in = rest[6:12]
    sems = [(rest[12 + 2 * i], rest[13 + 2 * i]) for i in range(8)]
    x1, x2, x3, m1, m2, m3, m3p, m4 = sems
    held, whole_sems, item_sems = rest[28:34], rest[34], rest[35]
    x_full, hid, hid_dot, grads, gate_in, upper_in = held

    me = lax.axis_index("gy")
    core, pair = lax.rem(me, 2), lax.div(me, 2)
    other = me + 1 - 2 * core
    peers = [lax.rem(pair + s, z.pairs) * 2 + core for s in range(1, z.pairs)]
    sources = [lax.rem(pair + z.pairs - s, z.pairs) * 2 + core for s in range(1, z.pairs)]
    hops = range(z.pairs - 1)

    up = Feed((w_gate, w_up, t_gate, t_up), up_slots, up_sems, z, lambda r, j: r.at[:, span(j, z.chunk)])
    down = Feed((w_down, t_down), down_slots, down_sems, z, lambda r, j: r.at[span(j, z.chunk), :])
    again = Feed((w_down, t_down), back_slots, back_sems, z, lambda r, j: r.at[span(j, z.chunk), :])

    def half_rows(k):
        return span(lax.div(k, z.steps), z.rows)

    def produce_up(k, part, slot):
        weights = up.take(k)
        x = x_full[half_rows(k), :]
        for i in range(4):
            part[i, slot] = matmul(x, weights[(0, 2, 1, 3)[i]])

    def combine_up(k, sums):
        gate, gate_dot, upper, upper_dot = sums
        for i in range(4):
            saved[i, k] = sums[i]
        silu_val, first, _ = silu_parts(gate)
        return (
            (silu_val * upper).astype(BF16),
            (first * gate_dot * upper + silu_val * upper_dot).astype(BF16),
        )

    def consume_up(k):
        weights = down.take(k)
        half, columns = lax.div(k, z.steps), span(lax.rem(k, z.steps), z.chunk)
        hidden, hidden_dot = hid[half_rows(k), columns], hid_dot[half_rows(k), columns]
        totals[half, 0] += matmul(hidden, weights[0])
        totals[half, 1] += matmul(hidden_dot, weights[0]) + matmul(hidden, weights[1])

    def produce_back(k, part, slot):
        weights = again.take(k)
        grad, grad_dot = grads[0, half_rows(k), :], grads[1, half_rows(k), :]
        part[0, slot] = tail_dot(grad, weights[0])
        part[1, slot] = tail_dot(grad_dot, weights[0]) + tail_dot(grad, weights[1])

    def combine_back(k, sums):
        back, back_dot = sums
        gate, gate_dot, upper, upper_dot = [saved[i, k] for i in range(4)]
        silu_val, first, second = silu_parts(gate)
        return (
            (
                back_dot * upper * first + back * upper_dot * first + back * upper * second * gate_dot
            ).astype(BF16),
            (back_dot * silu_val + back * first * gate_dot).astype(BF16),
        )

    def whole_out(i):
        return pltpu.make_async_copy(held[i], results[i], whole_sems.at[i])

    def item_out(i, k):
        block = (half_rows(k), span(lax.rem(k, z.steps), z.chunk))
        return pltpu.make_async_copy(
            held[4 + i].at[block], results[4 + i].at[block], item_sems.at[i, k]
        )

    def consume_back(k):
        for i in (0, 1):
            item_out(i, k).start()

    forward.bind(f_refs, hid, hid_dot, produce_up, combine_up, consume_up)
    backward.bind(b_refs, gate_in, upper_in, produce_back, combine_back, consume_back)

    barrier = pltpu.get_barrier_semaphore()

    def greet(axis, peer):
        pl.semaphore_signal(
            barrier, inc=1, device_id={axis: peer}, device_id_type=pl.DeviceIdType.MESH
        )

    greet("gx", forward.partner)
    pl.when(forward.spot > 0)(lambda: greet("gx", forward.me - 2))
    pl.when(forward.spot < forward.last)(lambda: greet("gx", forward.me + 2))
    for peer in [other, *peers]:
        greet("gy", peer)
    up.start(0)
    down.start(0)
    again.start(0)
    totals[...] = jnp.zeros_like(totals)
    pl.semaphore_wait(barrier, z.pairs + jnp.where(forward.at_end, 2, 3))

    def x_rows(h, index):
        return x_full.at[span(h * z.gy + index, z.own)]

    def x_copy(h, s):
        return remote(tokens.at[span(h, z.own)], x_rows(h, me), x1, (h, s), "gy", peers[s])

    def x_side(h):
        return remote(tokens.at[span(h, z.own)], x_rows(h, me), x2, h, "gy", other)

    def x_pass(h, s):
        block = x_rows(h, sources[s])
        return remote(block, block, x3, (h, s), "gy", other)

    for h in range(z.halves):
        for s in hops:
            x_copy(h, s).start()
        x_side(h).start()
        x_rows(h, me)[...] = tokens[h * z.own : (h + 1) * z.own, :]

    def x_relay(h):
        for s in hops:
            x_copy(h, s).wait_recv()
            x_pass(h, s).start()

    def x_take(h):
        x_side(h).wait_recv()
        for s in hops:
            x_pass(h, s).wait_recv()

    x_relay(0)
    x_take(0)

    def own_rows(index):
        return span(index, z.own)

    def m1_copy(h):
        return remote(m1_out.at[h], m1_in.at[h], m1, h, "gy", other)

    def m2_copy(h, s):
        return remote(m2_out.at[h, s], m2_in.at[h, s], m2, (h, s), "gy", peers[s])

    def grad_rows(h, index):
        return grads.at[:, span(h * z.gy + index, z.own), :]

    def m3_copy(h, s):
        return remote(grad_rows(h, me), grad_rows(h, me), m3, (h, s), "gy", peers[s])

    def m3_side(h):
        return remote(grad_rows(h, me), grad_rows(h, me), m3p, h, "gy", other)

    def m4_copy(h, s):
        block = grad_rows(h, sources[s])
        return remote(block, block, m4, (h, s), "gy", other)

    ready = z.steps - 1 + 2 * LAG_UP * z.line
    start_back = ready + MIDDLE[2]

    def middle_send(t):
        for h in range(z.halves):

            @pl.when(t == ready + h * z.steps)
            def _():
                for i in (0, 1):
                    for g in range(z.pairs):
                        m1_out[h, i, g] = totals[h, i, own_rows(g * 2 + 1 - core), :].astype(BF16)
                m1_copy(h).start()
                if h == z.halves - 1:
                    whole_out(1).start()
                    whole_out(2).start()

    def middle(t):
        for h in range(z.halves):
            base = ready + h * z.steps

            @pl.when(t == base + MIDDLE[0])
            def _():
                m1_copy(h).wait_recv()
                for i in (0, 1):
                    totals[h, i, own_rows(me), :] += m1_in[h, i, pair].astype(F32)
                for s in hops:
                    g = lax.div(peers[s], 2)
                    for i in (0, 1):
                        m2_out[h, s, i] = (
                            totals[h, i, own_rows(peers[s]), :] + m1_in[h, i, g].astype(F32)
                        ).astype(BF16)
                    m2_copy(h, s).start()

            @pl.when(t == base + MIDDLE[1])
            def _():
                outs = [totals[h, i, own_rows(me), :] for i in (0, 1)]
                for s in hops:
                    m2_copy(h, s).wait_recv()
                    outs = [outs[i] + m2_in[h, s, i].astype(F32) for i in (0, 1)]
                goal = target[h * z.own : (h + 1) * z.own, :].astype(F32)
                grad_rows(h, me)[0] = ((outs[0] - goal) * scale).astype(BF16)
                grad_rows(h, me)[1] = (outs[1] * scale).astype(BF16)
                for s in hops:
                    m3_copy(h, s).start()
                m3_side(h).start()

            @pl.when(t == base + MIDDLE[2])
            def _():
                for s in hops:
                    m3_copy(h, s).wait_recv()
                    m4_copy(h, s).start()

    def middle_take(t):
        for h in range(z.halves):

            @pl.when(t == ready + h * z.steps + MIDDLE[2])
            def _():
                m3_side(h).wait_recv()
                for s in hops:
                    m4_copy(h, s).wait_recv()
                if h == z.halves - 1:
                    whole_out(3).start()

    def x_later(t):
        for h in range(1, z.halves):
            pl.when(t == 1)(lambda: x_relay(h))
            pl.when(t == 3)(lambda: x_take(h))
        pl.when(t == 4)(lambda: whole_out(0).start())

    def step(t, carry):
        x_later(t)
        forward.early(t)
        middle(t)
        backward.early(t - start_back)
        forward.late(t)
        middle_send(t)
        middle_take(t)
        backward.late(t - start_back)
        return carry

    lax.fori_loop(0, start_back + z.items + 2 * LAG_BACK * z.line, step, 0)

    for h in range(z.halves):
        for s in hops:
            x_copy(h, s).wait_send()
            x_pass(h, s).wait_send()
            m2_copy(h, s).wait_send()
            m3_copy(h, s).wait_send()
            m4_copy(h, s).wait_send()
        x_side(h).wait_send()
        m1_copy(h).wait_send()
        m3_side(h).wait_send()

    def settle(k, carry):
        forward.settle(k)
        backward.settle(k)
        for i in (0, 1):
            item_out(i, k).wait()
        return carry

    lax.fori_loop(0, z.items, settle, 0)
    for i in range(4):
        whole_out(i).wait()


def run(tokens, target, w_gate, w_up, w_down, t_gate, t_up, t_down):
    z = Sizes(tokens, w_gate)
    model = w_down.shape[1]
    tall = z.halves * z.rows
    forward, backward = Stream(z, 2, 2, LAG_UP), Stream(z, 1, 1, LAG_BACK)
    vmem, any_spec = pl.BlockSpec(memory_space=pltpu.VMEM), pl.BlockSpec(memory_space=pl.ANY)
    sem = pltpu.SemaphoreType.DMA
    hops = max(z.pairs - 1, 1)
    wide = jax.ShapeDtypeStruct((tall, z.width), BF16)
    marks = [(z.halves, hops), (z.halves,), (z.halves, hops), (z.halves,), (z.halves, hops),
             (z.halves, hops), (z.halves,), (z.halves, hops)]
    outs = [
        jax.ShapeDtypeStruct((tall, z.depth), BF16),
        wide,
        wide,
        jax.ShapeDtypeStruct((2, tall, model), BF16),
        wide,
        wide,
    ]
    return pl.pallas_call(
        functools.partial(hvp_kernel, z, 1.0 / math.sqrt(TOKENS), forward, backward),
        out_shape=outs,
        in_specs=[vmem] * 2 + [any_spec] * 6,
        out_specs=[any_spec] * 6,
        scratch_shapes=[
            *forward.scratch(),
            *backward.scratch(),
            pltpu.VMEM((2, 4, z.depth, z.chunk), BF16),
            sem((2, 4)),
            pltpu.VMEM((2, 2, z.chunk, model), BF16),
            sem((2, 2)),
            pltpu.VMEM((2, 2, z.chunk, model), BF16),
            sem((2, 2)),
            pltpu.VMEM((z.halves, 2, z.rows, model), F32),
            pltpu.VMEM((4, z.items, z.group, z.chunk), F32),
            pltpu.VMEM((z.halves, 2, z.pairs, z.own, model), BF16),
            pltpu.VMEM((z.halves, 2, z.pairs, z.own, model), BF16),
            pltpu.VMEM((z.halves, hops, 2, z.own, model), BF16),
            pltpu.VMEM((z.halves, hops, 2, z.own, model), BF16),
            *[sem(shape) for shape in marks for _ in range(2)],
            *[pltpu.VMEM(out.shape, out.dtype) for out in outs],
            sem((4,)),
            sem((2, z.items)),
        ],
        compiler_params=pltpu.CompilerParams(
            collective_id=0, has_side_effects=True, vmem_limit_bytes=67043328
        ),
        cost_estimate=pl.CostEstimate(
            flops=20 * tall * z.depth * z.width,
            bytes_accessed=60 * tall * z.width,
            transcendentals=0,
        ),
    )(tokens, target, w_gate, w_up, t_gate, t_up, w_down, t_down)


def products_kernel(tokens, gate, upper, hidden, hidden_dot, grads, out_gate, out_up, out_down):
    out_gate[...] = lead_dot(tokens[...], gate[...]).astype(BF16)
    out_up[...] = lead_dot(tokens[...], upper[...]).astype(BF16)
    out_down[...] = (
        lead_dot(hidden_dot[...], grads[0]) + lead_dot(hidden[...], grads[1])
    ).astype(BF16)


def weight_products(tokens, gate, upper, hidden, hidden_dot, grads):
    rows, depth = tokens.shape
    width, model = gate.shape[1], grads.shape[2]
    tile = next(size for size in TILES if width % size == 0)
    strip = pl.BlockSpec((rows, tile), lambda i: (0, i))
    return pl.pallas_call(
        products_kernel,
        grid=(width // tile,),
        in_specs=[
            pl.BlockSpec((rows, depth), lambda i: (0, 0)),
            *[strip] * 4,
            pl.BlockSpec((2, rows, model), lambda i: (0, 0, 0)),
        ],
        out_specs=[
            pl.BlockSpec((depth, tile), lambda i: (0, i)),
            pl.BlockSpec((depth, tile), lambda i: (0, i)),
            pl.BlockSpec((tile, model), lambda i: (i, 0)),
        ],
        out_shape=[
            jax.ShapeDtypeStruct((depth, width), BF16),
            jax.ShapeDtypeStruct((depth, width), BF16),
            jax.ShapeDtypeStruct((width, model), BF16),
        ],
        cost_estimate=pl.CostEstimate(
            flops=4 * rows * (depth + model) * width,
            bytes_accessed=2 * (2 * depth + model + 4 * rows) * width,
            transcendentals=0,
        ),
    )(tokens, gate, upper, hidden, hidden_dot, grads)


def body(tokens, target, w_gate, w_up, w_down, t_gate, t_up, t_down):
    x_full, hidden, hidden_dot, grads, gate_in, upper_in = run(
        tokens, target, w_gate, w_up, w_down, t_gate, t_up, t_down
    )
    return tuple(weight_products(x_full, gate_in, upper_in, hidden, hidden_dot, grads))


def solution(mesh):
    return jax.shard_map(
        body,
        mesh=mesh,
        in_specs=(
            P("gy", "gx"),
            P("gy", "gx"),
            P("gx", "gy"),
            P("gx", "gy"),
            P("gy", "gx"),
            P("gx", "gy"),
            P("gx", "gy"),
            P("gy", "gx"),
        ),
        out_specs=(P("gx", "gy"), P("gx", "gy"), P("gy", "gx")),
        check_vma=False,
    )
```

```python
import functools
import math

import jax
import jax.numpy as jnp
from jax import lax
from jax.experimental import pallas as pl
from jax.experimental.pallas import tpu as pltpu
from jax.sharding import PartitionSpec as P

TOKENS = 256
CHUNKS = (512, 256, 128)
TILES = (896, 512, 256, 128)
LAG_UP, LAG_BACK = 2, 3
MIDDLE = (1, 3, 5)
F32, BF16 = jnp.float32, jnp.bfloat16


def silu_parts(gate):
    sig = jax.nn.sigmoid(gate)
    first = sig * (1.0 + gate * (1.0 - sig))
    second = sig * (1.0 - sig) * (2.0 + gate * (1.0 - 2.0 * sig))
    return (gate * sig, first, second)


def matmul(left, right):
    return jnp.dot(left, right, preferred_element_type=F32)


def lead_dot(left, right):
    return lax.dot_general(left, right, (((0,), (0,)), ((), ())), preferred_element_type=F32)


def tail_dot(left, right):
    return lax.dot_general(left, right, (((1,), (1,)), ((), ())), preferred_element_type=F32)


def between(value, low, high):
    return jnp.logical_and(value >= low, value < high)


def both(*terms):
    return functools.reduce(jnp.logical_and, terms)


def span(start, size):
    return pl.ds(pl.multiple_of(start * size, size), size)


def remote(src, dst, sems, index, axis, peer):
    return pltpu.make_async_remote_copy(
        src_ref=src,
        dst_ref=dst,
        send_sem=sems[0].at[index],
        recv_sem=sems[1].at[index],
        device_id={axis: peer},
        device_id_type=pl.DeviceIdType.MESH,
    )


class Sizes:
    def __init__(self, tokens, w_gate):
        self.line = lax.axis_size("gx") // 2
        self.gy = lax.axis_size("gy")
        self.pairs = self.gy // 2
        own, self.depth = tokens.shape
        self.width = w_gate.shape[1]
        self.halves = next(parts for parts in (4, 2, 1) if own % (16 * parts) == 0)
        self.own = own // self.halves
        self.rows = self.own * self.gy
        self.group = self.rows // 4
        self.chunk = next(size for size in CHUNKS if self.width % size == 0)
        self.steps = self.width // self.chunk
        self.items = self.halves * self.steps


class Stream:
    def __init__(self, sizes, na, nb, lag):
        self.z, self.na, self.nb, self.lag = sizes, na, nb, lag

    def scratch(self):
        z, na, nb = self.z, self.na, self.nb
        n, g, c = z.items, z.group, z.chunk
        sem = pltpu.SemaphoreType.DMA
        pairs = [(n,), (2, n), (2, n), (n,), (2, n), (2, n), (n,), (2, n)]
        return [
            pltpu.VMEM((na + nb, self.lag * z.line, z.rows, c), F32),
            pltpu.VMEM((n, na, 2, g, c), BF16),
            pltpu.VMEM((n, na, 2, g, c), BF16),
            pltpu.VMEM((2, n, na, g, c), BF16),
            pltpu.VMEM((2, n, nb, 2 * g, c), BF16),
            pltpu.VMEM((n, nb, g, c), BF16),
            pltpu.VMEM((n, nb, g, c), BF16),
            *[sem(shape) for shape in pairs for _ in range(2)],
        ]

    def bind(self, refs, full0, full1, produce, combine, consume):
        self.part, self.y_out, self.y_in, self.a, self.b, self.f_out, self.f_in = refs[:7]
        sems = [(refs[7 + 2 * i], refs[8 + 2 * i]) for i in range(8)]
        (self.ys, self.as_, self.bs, self.fs, self.hs, self.gs, self.xs, self.ks) = sems
        self.full0, self.full1 = full0, full1
        self.produce, self.combine, self.consume = produce, combine, consume
        z = self.z
        self.me = lax.axis_index("gx")
        self.spot, self.side = lax.div(self.me, 2), lax.rem(self.me, 2)
        self.partner = self.me + 1 - 2 * self.side
        self.last = z.line - 1
        self.at_end = jnp.logical_or(self.spot == 0, self.spot == self.last)
        self.end = jnp.where(self.spot == 0, 0, 1)
        self.place = [self.last - self.spot, self.spot]

    def group_of(self, e, s):
        return span(e * 2 + s, self.z.group)

    def block(self, full, k, e, s):
        z = self.z
        half, j = lax.div(k, z.steps), lax.rem(k, z.steps)
        return full.at[span(half * 4 + e * 2 + s, z.group), span(j, z.chunk)]

    def slab(self, full, k, e):
        z = self.z
        half, j = lax.div(k, z.steps), lax.rem(k, z.steps)
        return full.at[span(half * 2 + e, 2 * z.group), span(j, z.chunk)]

    def across(self, src, dst, sems, index):
        return remote(src, dst, sems, index, "gx", self.partner)

    def along(self, d, src, dst, sems, index):
        return remote(src, dst, sems, index, "gx", self.me - 2 + 4 * d)

    def y_copy(self, k):
        return self.across(self.y_out.at[k], self.y_in.at[k], self.ys, k)

    def f_copy(self, k):
        return self.across(self.f_out.at[k], self.f_in.at[k], self.fs, k)

    def a_copy(self, d, k):
        return self.along(d, self.a.at[d, k], self.a.at[d, k], self.as_, (d, k))

    def b_copy(self, d, k):
        return self.along(d, self.b.at[d, k], self.b.at[d, k], self.bs, (d, k))

    def h_copy(self, d, k):
        block = self.block(self.full0, k, 1 - d, self.side)
        return self.along(d, block, block, self.hs, (d, k))

    def g_copy(self, d, k):
        block = self.block(self.full0, k, 1 - d, self.side)
        return self.across(block, block, self.gs, (d, k))

    def x_copy(self, k):
        block = self.block(self.full1, k, self.end, self.side)
        return self.across(block, block, self.xs, k)

    def k_copy(self, d, k):
        block = self.slab(self.full1, k, 1 - d)
        return self.along(d, block, block, self.ks, (d, k))

    def early(self, t):
        z, last, side, na, nb = self.z, self.last, self.side, self.na, self.nb
        n, part, a, b = z.items, self.part, self.a, self.b
        for d in (0, 1):
            p = self.place[d]
            k, h = t - self.lag * (z.line + 1 + p), t - self.lag * (z.line + p)
            go = between(k, 0, n)

            @pl.when(both(go, p > 0))
            def _():
                self.k_copy(d, k).wait_recv()

            @pl.when(both(go, p == 0))
            def _():
                self.x_copy(k).wait_recv()

            @pl.when(both(go, p < last))
            def _():
                self.k_copy(d, k).start()

            @pl.when(both(between(h, 0, n), p > 0))
            def _():
                self.h_copy(d, h).wait_recv()
                self.g_copy(d, h).start()

            @pl.when(both(between(h, 0, n), between(p, 1, last)))
            def _():
                self.h_copy(d, h).start()

            @pl.when(go)
            def _():
                self.g_copy(d, k).wait_recv()

        k = t - self.lag * z.line

        @pl.when(both(between(k, 0, n), self.at_end))
        def _():
            self.a_copy(self.end, k).wait_recv()
            self.f_copy(k).wait_recv()
            slot, mine = lax.rem(k, self.lag * z.line), self.group_of(self.end, side)
            sums = [part[i, slot, mine, :] + a[self.end, k, i].astype(F32) for i in range(na)]
            sums += [part[na + i, slot, mine, :] + self.f_in[k, i].astype(F32) for i in range(nb)]
            first, second = self.combine(k, sums)
            self.block(self.full0, k, self.end, side)[...] = first
            self.block(self.full1, k, self.end, side)[...] = second
            self.x_copy(k).start()
            self.h_copy(1 - self.end, k).start()
            self.g_copy(1 - self.end, k).start()

        for d in (0, 1):
            p = self.place[d]
            k = t - self.lag * p

            @pl.when(both(between(k, 0, n), between(p, 1, last)))
            def _():
                self.b_copy(d, k).wait_recv()
                slot, slab = lax.rem(k, self.lag * z.line), span(d, 2 * z.group)
                for i in range(nb):
                    b[d, k, i] = (part[na + i, slot, slab, :] + b[d, k, i].astype(F32)).astype(BF16)
                self.b_copy(d, k).start()

            @pl.when(both(between(k, 0, n), p == last))
            def _():
                self.b_copy(d, k).wait_recv()
                slot = lax.rem(k, self.lag * z.line)
                own, other = span(side, z.group), span(1 - side, z.group)
                for i in range(nb):
                    self.f_out[k, i] = (
                        part[na + i, slot, self.group_of(d, 1 - side), :]
                        + b[d, k, i, other, :].astype(F32)
                    ).astype(BF16)
                self.f_copy(k).start()
                for i in range(nb):
                    part[na + i, slot, self.group_of(d, side), :] += b[d, k, i, own, :].astype(F32)

        k = t - self.lag

        @pl.when(between(k, 0, n))
        def _():
            self.y_copy(k).wait_recv()
            for i in range(na):
                for e in (0, 1):
                    part[i, lax.rem(k, self.lag * z.line), self.group_of(e, side), :] += self.y_in[
                        k, i, e
                    ].astype(F32)

        for d in (0, 1):
            p = self.place[d]
            k = t - self.lag * (1 + p)

            @pl.when(both(between(k, 0, n), between(p, 1, last)))
            def _():
                self.a_copy(d, k).wait_recv()
                for i in range(na):
                    a[d, k, i] = (
                        part[i, lax.rem(k, self.lag * z.line), self.group_of(d, side), :]
                        + a[d, k, i].astype(F32)
                    ).astype(BF16)
                self.a_copy(d, k).start()

            @pl.when(both(between(k, 0, n), p == 0))
            def _():
                for i in range(na):
                    a[d, k, i] = part[i, lax.rem(k, self.lag * z.line), self.group_of(d, side), :].astype(BF16)
                self.a_copy(d, k).start()

    def late(self, t):
        z, na, nb = self.z, self.na, self.nb

        @pl.when(between(t, 0, z.items))
        def _():
            slot = lax.rem(t, self.lag * z.line)
            self.produce(t, self.part, slot)
            for i in range(na):
                for e in (0, 1):
                    self.y_out[t, i, e] = self.part[
                        i, slot, self.group_of(e, 1 - self.side), :
                    ].astype(BF16)
            self.y_copy(t).start()

            @pl.when(self.at_end)
            def _():
                d = 1 - self.end
                for i in range(nb):
                    self.b[d, t, i] = self.part[na + i, slot, span(d, 2 * z.group), :].astype(BF16)
                self.b_copy(d, t).start()

        if self.consume is not None:
            k = t - 2 * self.lag * z.line

            @pl.when(between(k, 0, z.items))
            def _():
                self.consume(k)

    def settle(self, k):
        self.y_copy(k).wait_send()

        @pl.when(self.at_end)
        def _():
            self.f_copy(k).wait_send()
            self.x_copy(k).wait_send()

        for d in (0, 1):
            self.g_copy(d, k).wait_send()

            @pl.when(self.place[d] < self.last)
            def _():
                self.a_copy(d, k).wait_send()
                self.b_copy(d, k).wait_send()
                self.h_copy(d, k).wait_send()
                self.k_copy(d, k).wait_send()


class Feed:
    def __init__(self, sources, slots, sems, sizes, view):
        self.sources, self.slots, self.sems = sources, slots, sems
        self.sizes, self.view = sizes, view

    def copies(self, k):
        slot, j = lax.rem(k, 2), lax.rem(k, self.sizes.steps)
        return [
            pltpu.make_async_copy(
                self.view(source, j), self.slots.at[slot, i], self.sems.at[slot, i]
            )
            for i, source in enumerate(self.sources)
        ]

    def start(self, k):
        for copy in self.copies(k):
            copy.start()

    def take(self, k):
        for copy in self.copies(k):
            copy.wait()
        pl.when(k + 1 < self.sizes.items)(lambda: self.start(k + 1))
        return self.slots.at[lax.rem(k, 2)]


def hvp_kernel(z, scale, forward, backward, *refs):
    tokens, target, w_gate, w_up, t_gate, t_up, w_down, t_down = refs[:8]
    results = refs[8:14]
    count = len(forward.scratch())
    f_refs, b_refs, rest = refs[14 : 14 + count], refs[14 + count : 14 + 2 * count], refs[14 + 2 * count :]
    up_slots, up_sems, down_slots, down_sems, back_slots, back_sems = rest[:6]
    totals, saved, m1_out, m1_in, m2_out, m2_in = rest[6:12]
    sems = [(rest[12 + 2 * i], rest[13 + 2 * i]) for i in range(8)]
    x1, x2, x3, m1, m2, m3, m3p, m4 = sems
    held, whole_sems, item_sems = rest[28:34], rest[34], rest[35]
    x_full, hid, hid_dot, grads, gate_in, upper_in = held

    me = lax.axis_index("gy")
    core, pair = lax.rem(me, 2), lax.div(me, 2)
    other = me + 1 - 2 * core
    peers = [lax.rem(pair + s, z.pairs) * 2 + core for s in range(1, z.pairs)]
    sources = [lax.rem(pair + z.pairs - s, z.pairs) * 2 + core for s in range(1, z.pairs)]
    hops = range(z.pairs - 1)

    up = Feed((w_gate, w_up, t_gate, t_up), up_slots, up_sems, z, lambda r, j: r.at[:, span(j, z.chunk)])
    down = Feed((w_down, t_down), down_slots, down_sems, z, lambda r, j: r.at[span(j, z.chunk), :])
    again = Feed((w_down, t_down), back_slots, back_sems, z, lambda r, j: r.at[span(j, z.chunk), :])

    def half_rows(k):
        return span(lax.div(k, z.steps), z.rows)

    def produce_up(k, part, slot):
        weights = up.take(k)
        x = x_full[half_rows(k), :]
        for i in range(4):
            part[i, slot] = matmul(x, weights[(0, 2, 1, 3)[i]])

    def combine_up(k, sums):
        gate, gate_dot, upper, upper_dot = sums
        for i in range(4):
            saved[i, k] = sums[i]
        silu_val, first, _ = silu_parts(gate)
        return (
            (silu_val * upper).astype(BF16),
            (first * gate_dot * upper + silu_val * upper_dot).astype(BF16),
        )

    def consume_up(k):
        weights = down.take(k)
        half, columns = lax.div(k, z.steps), span(lax.rem(k, z.steps), z.chunk)
        hidden, hidden_dot = hid[half_rows(k), columns], hid_dot[half_rows(k), columns]
        joint = matmul(jnp.concatenate([hidden, hidden_dot], axis=0), weights[0])
        totals[half, 0] += joint[: z.rows]
        totals[half, 1] += joint[z.rows :] + matmul(hidden, weights[1])

    def produce_back(k, part, slot):
        weights = again.take(k)
        grad, grad_dot = grads[0, half_rows(k), :], grads[1, half_rows(k), :]
        joint = tail_dot(jnp.concatenate([grad, grad_dot], axis=0), weights[0])
        part[0, slot] = joint[: z.rows]
        part[1, slot] = joint[z.rows :] + tail_dot(grad, weights[1])

    def combine_back(k, sums):
        back, back_dot = sums
        gate, gate_dot, upper, upper_dot = [saved[i, k] for i in range(4)]
        silu_val, first, second = silu_parts(gate)
        return (
            (
                back_dot * upper * first + back * upper_dot * first + back * upper * second * gate_dot
            ).astype(BF16),
            (back_dot * silu_val + back * first * gate_dot).astype(BF16),
        )

    def whole_out(i):
        return pltpu.make_async_copy(held[i], results[i], whole_sems.at[i])

    def item_out(i, k):
        block = (half_rows(k), span(lax.rem(k, z.steps), z.chunk))
        return pltpu.make_async_copy(
            held[4 + i].at[block], results[4 + i].at[block], item_sems.at[i, k]
        )

    def consume_back(k):
        for i in (0, 1):
            item_out(i, k).start()

    forward.bind(f_refs, hid, hid_dot, produce_up, combine_up, consume_up)
    backward.bind(b_refs, gate_in, upper_in, produce_back, combine_back, consume_back)

    barrier = pltpu.get_barrier_semaphore()

    def greet(axis, peer):
        pl.semaphore_signal(
            barrier, inc=1, device_id={axis: peer}, device_id_type=pl.DeviceIdType.MESH
        )

    greet("gx", forward.partner)
    pl.when(forward.spot > 0)(lambda: greet("gx", forward.me - 2))
    pl.when(forward.spot < forward.last)(lambda: greet("gx", forward.me + 2))
    for peer in [other, *peers]:
        greet("gy", peer)
    up.start(0)
    down.start(0)
    again.start(0)
    totals[...] = jnp.zeros_like(totals)
    pl.semaphore_wait(barrier, z.pairs + jnp.where(forward.at_end, 2, 3))

    def x_rows(h, index):
        return x_full.at[span(h * z.gy + index, z.own)]

    def x_copy(h, s):
        return remote(tokens.at[span(h, z.own)], x_rows(h, me), x1, (h, s), "gy", peers[s])

    def x_side(h):
        return remote(tokens.at[span(h, z.own)], x_rows(h, me), x2, h, "gy", other)

    def x_pass(h, s):
        block = x_rows(h, sources[s])
        return remote(block, block, x3, (h, s), "gy", other)

    for h in range(z.halves):
        for s in hops:
            x_copy(h, s).start()
        x_side(h).start()
        x_rows(h, me)[...] = tokens[h * z.own : (h + 1) * z.own, :]

    def x_relay(h):
        for s in hops:
            x_copy(h, s).wait_recv()
            x_pass(h, s).start()

    def x_take(h):
        x_side(h).wait_recv()
        for s in hops:
            x_pass(h, s).wait_recv()

    x_relay(0)
    x_take(0)

    def own_rows(index):
        return span(index, z.own)

    def m1_copy(h):
        return remote(m1_out.at[h], m1_in.at[h], m1, h, "gy", other)

    def m2_copy(h, s):
        return remote(m2_out.at[h, s], m2_in.at[h, s], m2, (h, s), "gy", peers[s])

    def grad_rows(h, index):
        return grads.at[:, span(h * z.gy + index, z.own), :]

    def m3_copy(h, s):
        return remote(grad_rows(h, me), grad_rows(h, me), m3, (h, s), "gy", peers[s])

    def m3_side(h):
        return remote(grad_rows(h, me), grad_rows(h, me), m3p, h, "gy", other)

    def m4_copy(h, s):
        block = grad_rows(h, sources[s])
        return remote(block, block, m4, (h, s), "gy", other)

    ready = z.steps - 1 + 2 * LAG_UP * z.line
    start_back = ready + MIDDLE[2]

    def middle_send(t):
        for h in range(z.halves):

            @pl.when(t == ready + h * z.steps)
            def _():
                for i in (0, 1):
                    for g in range(z.pairs):
                        m1_out[h, i, g] = totals[h, i, own_rows(g * 2 + 1 - core), :].astype(BF16)
                m1_copy(h).start()
                if h == z.halves - 1:
                    whole_out(1).start()
                    whole_out(2).start()

    def middle(t):
        for h in range(z.halves):
            base = ready + h * z.steps

            @pl.when(t == base + MIDDLE[0])
            def _():
                m1_copy(h).wait_recv()
                for i in (0, 1):
                    totals[h, i, own_rows(me), :] += m1_in[h, i, pair].astype(F32)
                for s in hops:
                    g = lax.div(peers[s], 2)
                    for i in (0, 1):
                        m2_out[h, s, i] = (
                            totals[h, i, own_rows(peers[s]), :] + m1_in[h, i, g].astype(F32)
                        ).astype(BF16)
                    m2_copy(h, s).start()

            @pl.when(t == base + MIDDLE[1])
            def _():
                outs = [totals[h, i, own_rows(me), :] for i in (0, 1)]
                for s in hops:
                    m2_copy(h, s).wait_recv()
                    outs = [outs[i] + m2_in[h, s, i].astype(F32) for i in (0, 1)]
                goal = target[h * z.own : (h + 1) * z.own, :].astype(F32)
                grad_rows(h, me)[0] = ((outs[0] - goal) * scale).astype(BF16)
                grad_rows(h, me)[1] = (outs[1] * scale).astype(BF16)
                for s in hops:
                    m3_copy(h, s).start()
                m3_side(h).start()

            @pl.when(t == base + MIDDLE[2])
            def _():
                for s in hops:
                    m3_copy(h, s).wait_recv()
                    m4_copy(h, s).start()

    def middle_take(t):
        for h in range(z.halves):

            @pl.when(t == ready + h * z.steps + MIDDLE[2])
            def _():
                m3_side(h).wait_recv()
                for s in hops:
                    m4_copy(h, s).wait_recv()
                if h == z.halves - 1:
                    whole_out(3).start()

    def x_later(t):
        for h in range(1, z.halves):
            pl.when(t == 1)(lambda: x_relay(h))
            pl.when(t == 3)(lambda: x_take(h))
        pl.when(t == 4)(lambda: whole_out(0).start())

    def step(t, carry):
        x_later(t)
        forward.early(t)
        middle(t)
        backward.early(t - start_back)
        forward.late(t)
        middle_send(t)
        middle_take(t)
        backward.late(t - start_back)
        return carry

    lax.fori_loop(0, start_back + z.items + 2 * LAG_BACK * z.line, step, 0)

    for h in range(z.halves):
        for s in hops:
            x_copy(h, s).wait_send()
            x_pass(h, s).wait_send()
            m2_copy(h, s).wait_send()
            m3_copy(h, s).wait_send()
            m4_copy(h, s).wait_send()
        x_side(h).wait_send()
        m1_copy(h).wait_send()
        m3_side(h).wait_send()

    def settle(k, carry):
        forward.settle(k)
        backward.settle(k)
        for i in (0, 1):
            item_out(i, k).wait()
        return carry

    lax.fori_loop(0, z.items, settle, 0)
    for i in range(4):
        whole_out(i).wait()


def run(tokens, target, w_gate, w_up, w_down, t_gate, t_up, t_down):
    z = Sizes(tokens, w_gate)
    model = w_down.shape[1]
    tall = z.halves * z.rows
    forward, backward = Stream(z, 2, 2, LAG_UP), Stream(z, 1, 1, LAG_BACK)
    vmem, any_spec = pl.BlockSpec(memory_space=pltpu.VMEM), pl.BlockSpec(memory_space=pl.ANY)
    sem = pltpu.SemaphoreType.DMA
    hops = max(z.pairs - 1, 1)
    wide = jax.ShapeDtypeStruct((tall, z.width), BF16)
    marks = [(z.halves, hops), (z.halves,), (z.halves, hops), (z.halves,), (z.halves, hops),
             (z.halves, hops), (z.halves,), (z.halves, hops)]
    outs = [
        jax.ShapeDtypeStruct((tall, z.depth), BF16),
        wide,
        wide,
        jax.ShapeDtypeStruct((2, tall, model), BF16),
        wide,
        wide,
    ]
    return pl.pallas_call(
        functools.partial(hvp_kernel, z, 1.0 / math.sqrt(TOKENS), forward, backward),
        out_shape=outs,
        in_specs=[vmem] * 2 + [any_spec] * 6,
        out_specs=[any_spec] * 6,
        scratch_shapes=[
            *forward.scratch(),
            *backward.scratch(),
            pltpu.VMEM((2, 4, z.depth, z.chunk), BF16),
            sem((2, 4)),
            pltpu.VMEM((2, 2, z.chunk, model), BF16),
            sem((2, 2)),
            pltpu.VMEM((2, 2, z.chunk, model), BF16),
            sem((2, 2)),
            pltpu.VMEM((z.halves, 2, z.rows, model), F32),
            pltpu.VMEM((4, z.items, z.group, z.chunk), F32),
            pltpu.VMEM((z.halves, 2, z.pairs, z.own, model), BF16),
            pltpu.VMEM((z.halves, 2, z.pairs, z.own, model), BF16),
            pltpu.VMEM((z.halves, hops, 2, z.own, model), BF16),
            pltpu.VMEM((z.halves, hops, 2, z.own, model), BF16),
            *[sem(shape) for shape in marks for _ in range(2)],
            *[pltpu.VMEM(out.shape, out.dtype) for out in outs],
            sem((4,)),
            sem((2, z.items)),
        ],
        compiler_params=pltpu.CompilerParams(
            collective_id=0, has_side_effects=True, vmem_limit_bytes=67043328
        ),
        cost_estimate=pl.CostEstimate(
            flops=20 * tall * z.depth * z.width,
            bytes_accessed=60 * tall * z.width,
            transcendentals=0,
        ),
    )(tokens, target, w_gate, w_up, t_gate, t_up, w_down, t_down)


def products_kernel(tokens, gate, upper, hidden, hidden_dot, grads, out_gate, out_up, out_down):
    out_gate[...] = lead_dot(tokens[...], gate[...]).astype(BF16)
    out_up[...] = lead_dot(tokens[...], upper[...]).astype(BF16)
    out_down[...] = (
        lead_dot(hidden_dot[...], grads[0]) + lead_dot(hidden[...], grads[1])
    ).astype(BF16)


def weight_products(tokens, gate, upper, hidden, hidden_dot, grads):
    rows, depth = tokens.shape
    width, model = gate.shape[1], grads.shape[2]
    tile = next(size for size in TILES if width % size == 0)
    strip = pl.BlockSpec((rows, tile), lambda i: (0, i))
    return pl.pallas_call(
        products_kernel,
        grid=(width // tile,),
        in_specs=[
            pl.BlockSpec((rows, depth), lambda i: (0, 0)),
            *[strip] * 4,
            pl.BlockSpec((2, rows, model), lambda i: (0, 0, 0)),
        ],
        out_specs=[
            pl.BlockSpec((depth, tile), lambda i: (0, i)),
            pl.BlockSpec((depth, tile), lambda i: (0, i)),
            pl.BlockSpec((tile, model), lambda i: (i, 0)),
        ],
        out_shape=[
            jax.ShapeDtypeStruct((depth, width), BF16),
            jax.ShapeDtypeStruct((depth, width), BF16),
            jax.ShapeDtypeStruct((width, model), BF16),
        ],
        cost_estimate=pl.CostEstimate(
            flops=4 * rows * (depth + model) * width,
            bytes_accessed=2 * (2 * depth + model + 4 * rows) * width,
            transcendentals=0,
        ),
    )(tokens, gate, upper, hidden, hidden_dot, grads)


def body(tokens, target, w_gate, w_up, w_down, t_gate, t_up, t_down):
    x_full, hidden, hidden_dot, grads, gate_in, upper_in = run(
        tokens, target, w_gate, w_up, w_down, t_gate, t_up, t_down
    )
    return tuple(weight_products(x_full, gate_in, upper_in, hidden, hidden_dot, grads))


def solution(mesh):
    return jax.shard_map(
        body,
        mesh=mesh,
        in_specs=(
            P("gy", "gx"),
            P("gy", "gx"),
            P("gx", "gy"),
            P("gx", "gy"),
            P("gy", "gx"),
            P("gx", "gy"),
            P("gx", "gy"),
            P("gy", "gx"),
        ),
        out_specs=(P("gx", "gy"), P("gx", "gy"), P("gy", "gx")),
        check_vma=False,
    )
```
